32 devices in a mesh: groups: 2 (over y), seq: 4 (over z), head: 4 (over x, core).
Axes of the slice: x: 2, y: 2, z: 4, core: 2. Of those that a mesh axis runs over, the one named last changes fastest.
Arguments:
- tokens: bfloat16 [4096, 4096], P(('groups', 'seq')), parts along dimension 0, may hold values from -24 to 24
- proj_weight: bfloat16 [3, 4096, 2048], P(None, 'seq', 'head'), may hold values from -1 to 1
- cluster_ids: int32 [16, 4096, 1], P('head', ('groups', 'seq')), parts along dimension 1, may hold values from 0 to 255; in each aligned block of 512 rows (0 to 511, 512 to 1023, ..., all dimensions but the last counted through in order) at most 4 rows name the same one
- centroids: float32 [32, 256, 128], P(('groups', 'head'), 'seq'), parts along dimension 0, may hold values from -3 to 3
Outputs:
- context: bfloat16 [4096, 2048], P(('groups', 'seq'), 'head'), parts along dimension 0
- new_centroids: float32 [32, 256, 128], P(('groups', 'head'), 'seq'), parts along dimension 0
The draws below stay inside these ranges and needn't reach their ends.
There are 2 independent parts, one for each index of `groups`. The reference program is written for one: setup_inputs(seed, part) draws one part's arguments, and reference() takes and returns one part's arrays. A program takes and returns all parts, laid end to end along the dimension named above; an argument that names none is the same for every part. Nothing has to cross between parts.
Inputs may be any that keep to these rules, and one draw needn't show every extreme that they name: `cluster_ids`: for each head, no cluster is named by more than 4 of the 512 tokens of one aligned block (one index of seq); some blocks reach 4.
All inputs are finite; a program needn't handle non-finite values.
Results may differ from the reference program's by a relative error of at most 0.018.
Values may be sent and summed in bfloat16 or wider, within the bound.
No kernel may reach another device: no remote copies, remote signals or barrier semaphores. Data moves between devices by JAX's collectives and lax.ppermute only.
A program may use at most 64 MiB of HBM per device.

```python
import math
import jax
import jax.numpy as jnp
import numpy as np
from jax import lax

D = 4096
HEADS = 16
HS = 128
CLUSTERS = 256
TOK_DEV = 512
SLOTS = 4
TOKENS = 2048
N_SEQ = 4


def draw_tokens(key, part):
    values_base = jnp.clip(jax.random.normal(jax.random.fold_in(key, 11), (TOKENS, D), jnp.float32), -4.0, 4.0)
    return values_base.astype(jnp.bfloat16)


def draw_proj_weight(key, part):
    drawn = jnp.clip(jax.random.normal(jax.random.fold_in(key, 21), (3, D, HEADS * HS), jnp.float32), -4.0, 4.0) * D ** (-0.5)
    return drawn.astype(jnp.bfloat16)


def block_levels(rng, shape, cuts, low, high):
    def one(axis_at, blocks):
        heights = jax.random.uniform(jax.random.fold_in(jax.random.fold_in(rng, 6), axis_at), (blocks,), jnp.float32, low / len(cuts), high / len(cuts))
        return jnp.repeat(jnp.exp(heights), shape[axis_at] // blocks).reshape((-1,) + (1,) * (len(shape) - axis_at - 1))

    factor_of = one(*cuts[0])
    for cut in cuts[1:]:
        factor_of = factor_of * one(*cut)
    return factor_of


def routed_block(stream_key, own, number, rows, count, top, reach, skew):
    order = jax.random.permutation(stream_key, count)
    heavy_load, ordinary = load_shares(count, rows * top, reach, skew, True), load_shares(count, rows * top, reach, skew, False)
    places = jnp.arange(count)

    def named(sizes, rotation):
        used = int((sizes > 0).sum())
        fixed = max(1, used // 4)
        shifted = fixed + (places - fixed + rotation * (used - fixed)) % max(1, count - fixed)
        return jnp.zeros((count,), jnp.int32).at[order[jnp.where(places < fixed, places, shifted)]].set(jnp.asarray(sizes, jnp.int32))

    sizes = jnp.where(number % 4 == 0, named(heavy_load, number // 4), named(ordinary, number - number // 4 - 1))
    mixed = jax.random.permutation(jax.random.fold_in(own, 3), count)
    donor, taker = mixed[0:count // 2 * 2:2], mixed[1:count // 2 * 2:2]
    room = jnp.minimum(sizes[donor] - 1, reach - sizes[taker]) // 2
    room = jnp.where((donor == order[0]) | (taker == order[0]) | (sizes[taker] == 0), 0, jnp.maximum(room, 0))
    shifted = jax.random.randint(jax.random.fold_in(own, 4), (count // 2,), 0, 1 << 20) % (room + 1)
    sizes = sizes.at[donor].add(-shifted).at[taker].add(shifted)
    items = jnp.searchsorted(jnp.cumsum(sizes), jnp.arange(rows * top), side="right").astype(jnp.int32)
    grid = items.reshape(top, rows).T
    grid = grid[jax.random.permutation(jax.random.fold_in(own, 1), rows)]
    rotation = jax.random.randint(jax.random.fold_in(own, 2), (rows, 1), 0, top)
    return jnp.take_along_axis(grid, (jnp.arange(top)[None, :] + rotation) % top, axis=1)


def load_shares(number_of, total, most, lean, full):
    weights = [(1 << 20) // math.isqrt(rank ** lean) + 1 for rank in range(1, number_of + 1)]
    largest = most if full else min(most, max(-(-total // number_of), total * weights[0] // sum(weights)))
    least = 1 if total - largest >= number_of - 1 else 0
    given, surplus = [largest] + [least] * (number_of - 1), total - largest - least * (number_of - 1)
    while surplus > 0:
        movable = [i for i in range(1, number_of) if given[i] < largest] or [i for i in range(1, number_of) if given[i] < most]
        mass, remaining = sum([weights[i] for i in movable]), surplus
        for i in movable:
            addition = min(most - given[i], max(1, remaining * weights[i] // mass), surplus)
            given[i] = given[i] + addition
            surplus = surplus - addition
    return np.array(given)


def centred(key, dims, width, bound, shards=(), held_as=jnp.bfloat16):
    result = width * jax.random.normal(key, dims, jnp.float32)
    if shards:
        result = result * block_levels(key, dims, shards, -0.22, 0.18)
    return jnp.clip(result, -bound, bound).astype(held_as)


def setup_inputs(seed: int = 0, part: int = 0) -> dict:
    key_list = jax.random.split(jax.random.key(seed), 5)
    part_splits = jax.random.split(jax.random.fold_in(key_list[4], part), 5)
    tokens = draw_tokens(jax.random.fold_in(jax.random.fold_in(key_list[4], part), 71), part)
    proj_weight = draw_proj_weight(jax.random.fold_in(key_list[4], 71), part)
    cluster_ids_keys = jax.random.split(jax.random.fold_in(part_splits[2], 1), HEADS * TOKENS // TOK_DEV)
    cluster_ids_turns = jax.random.permutation(jax.random.fold_in(part_splits[2], 3), HEADS * TOKENS // TOK_DEV)
    cluster_ids = jax.vmap(lambda own, number: routed_block(jax.random.fold_in(part_splits[2], 2), own, number, TOK_DEV, CLUSTERS, 1, SLOTS, 2))(cluster_ids_keys, cluster_ids_turns).reshape((HEADS, TOKENS, 1))
    centroids = centred(part_splits[3], (HEADS, CLUSTERS, HS), 0.5, 3.0, ((0, 4), (1, 4)), jnp.float32)
    return {"tokens": tokens, "proj_weight": proj_weight, "cluster_ids": cluster_ids, "centroids": centroids}


def one_head(inputs):
    queries, key_rows, value_rows, member, current = inputs
    capacity = N_SEQ * SLOTS
    labels = jnp.arange(CLUSTERS, dtype=jnp.int32)
    onehot = (member[:, None] == labels[None, :]).astype(jnp.int32)
    blocks = onehot.reshape(N_SEQ, TOK_DEV, CLUSTERS)
    prior = (jnp.cumsum(blocks, axis=1) - blocks).reshape(TOKENS, CLUSTERS).astype(jnp.int32)
    ranking = jnp.sum(prior * onehot, axis=1).astype(jnp.int32)
    source = jnp.arange(TOKENS, dtype=jnp.int32) // TOK_DEV
    slot_index = (source * SLOTS + ranking).astype(jnp.int32)
    packed = jnp.concatenate([queries, key_rows, value_rows], axis=1)
    outbox = jnp.zeros((CLUSTERS, capacity, 3 * HS), jnp.bfloat16).at[member, slot_index].set(packed)
    filled = jnp.zeros((CLUSTERS, capacity), jnp.int32).at[member, slot_index].set(1)
    query_block = outbox[:, :, :HS].astype(jnp.float32)
    key_block = outbox[:, :, HS:2 * HS].astype(jnp.float32)
    value_block = outbox[:, :, 2 * HS:].astype(jnp.float32)
    scores = jnp.einsum("cqd,ckd->cqk", query_block, key_block, precision=lax.Precision.HIGHEST) * (HS ** -0.5)
    ordinal = jnp.arange(capacity, dtype=jnp.int32)
    allowed = ((filled[:, None, :] > 0) & (ordinal[None, None, :] <= ordinal[None, :, None])) | (ordinal[None, None, :] == ordinal[None, :, None])
    scores = jnp.where(allowed, scores, -1e30)
    row_max = jnp.max(scores, axis=2, keepdims=True)
    raised = jnp.exp(scores - row_max)
    weights = (raised / jnp.sum(raised, axis=2, keepdims=True)).astype(jnp.bfloat16)
    attended = jnp.einsum("cqk,ckd->cqd", weights.astype(jnp.float32), value_block, precision=lax.Precision.HIGHEST).astype(jnp.bfloat16)
    context = attended[member, slot_index]
    key_sums = jnp.dot(onehot.astype(jnp.float32).T, key_rows.astype(jnp.float32), precision=lax.Precision.HIGHEST)
    counts = jnp.sum(onehot, axis=0).astype(jnp.float32)
    updated = 0.25 * current + 0.75 * key_sums / jnp.maximum(counts, 1.0)[:, None]
    return context, updated


def reference(tokens, proj_weight, cluster_ids, centroids):
    stacked = []
    for which in range(3):
        projected = jnp.dot(tokens, proj_weight[which], preferred_element_type=jnp.float32).astype(jnp.bfloat16)
        stacked.append(projected.reshape(TOKENS, HEADS, HS).transpose(1, 0, 2))
    contexts, updated = lax.map(one_head, (stacked[0], stacked[1], stacked[2], cluster_ids[:, :, 0], centroids))
    context = contexts.transpose(1, 0, 2).reshape(TOKENS, HEADS * HS)
    return context, updated
```

```python
import jax
import jax.numpy as jnp
from jax import lax
from jax.experimental import pallas as pl
from jax.experimental.pallas import tpu as pltpu
from jax.sharding import PartitionSpec as P

SLOTS = 4
CORES = 2


def routed(tokens, proj_weight, cluster_ids, centroids):
    owners = lax.axis_size("seq")
    local_rows = tokens.shape[0]
    hs = centroids.shape[2]
    clusters = centroids.shape[1] * owners
    columns = proj_weight.shape[2]
    head_count = columns // hs
    owned = clusters // owners
    capacity = owners * SLOTS
    score_scale = hs ** (-0.5)
    projected = jnp.einsum(
        "td,pdc->ptc",
        tokens,
        lax.all_gather(proj_weight, "seq", axis=1, tiled=True),
        preferred_element_type=jnp.float32,
    ).astype(jnp.bfloat16)
    per_head = projected.reshape(3, local_rows, head_count, hs).transpose(2, 1, 0, 3)
    packed = per_head.reshape(head_count, local_rows, 3 * hs)
    member = cluster_ids[:, :, 0]
    labels = jnp.arange(clusters, dtype=jnp.int32)
    onehot = (member[:, :, None] == labels[None, None, :]).astype(jnp.bfloat16)
    ordinal_rows = jnp.arange(local_rows, dtype=jnp.int32)
    earlier = (ordinal_rows[None, :] < ordinal_rows[:, None]).astype(jnp.bfloat16)
    before = jnp.einsum("ts,hsc->htc", earlier, onehot, preferred_element_type=jnp.float32)
    ranking = jnp.take_along_axis(before, member[:, :, None], axis=2)[:, :, 0].astype(jnp.int32)
    placed = member * SLOTS + ranking
    head_index = jnp.arange(head_count, dtype=jnp.int32)[:, None]
    outbox = (
        jnp.zeros((head_count, clusters * SLOTS, 3 * hs), jnp.bfloat16)
        .at[head_index, placed]
        .set(packed)
    )
    outbox = outbox.reshape(head_count, owners, owned * SLOTS, 3 * hs)
    local_counts = jnp.sum(onehot, axis=1, dtype=jnp.float32)
    tallies = local_counts.astype(jnp.int32).reshape(head_count, owners, owned)
    blocks = lax.all_to_all(outbox, "seq", split_axis=1, concat_axis=1, tiled=True)
    arrived = lax.all_to_all(tallies, "seq", split_axis=1, concat_axis=1, tiled=True)
    arranged = (
        blocks.reshape(head_count, owners, owned, SLOTS, 3 * hs)
        .transpose(0, 2, 1, 3, 4)
        .reshape(head_count, owned, capacity, 3 * hs)
    )
    filled = jnp.arange(SLOTS, dtype=jnp.int32)[None, None, None, :] < arrived[:, :, :, None]
    filled = filled.transpose(0, 2, 1, 3).reshape(head_count, owned, capacity)
    queries = arranged[:, :, :, :hs]
    key_block = arranged[:, :, :, hs : 2 * hs]
    value_block = arranged[:, :, :, 2 * hs :]
    scores = (
        jnp.einsum("hcqd,hckd->hcqk", queries, key_block, preferred_element_type=jnp.float32)
        * score_scale
    )
    ordinal = jnp.arange(capacity, dtype=jnp.int32)
    causal = ordinal[None, None, None, :] <= ordinal[None, None, :, None]
    itself = ordinal[None, None, None, :] == ordinal[None, None, :, None]
    allowed = filled[:, :, None, :] & causal | itself
    scores = jnp.where(allowed, scores, -1e30)
    row_max = jnp.max(scores, axis=3, keepdims=True)
    raised = jnp.exp(scores - row_max)
    weights = (raised / jnp.sum(raised, axis=3, keepdims=True)).astype(jnp.bfloat16)
    attended = jnp.einsum(
        "hcqk,hckd->hcqd", weights, value_block, preferred_element_type=jnp.float32
    ).astype(jnp.bfloat16)
    attended = (
        attended.reshape(head_count, owned, owners, SLOTS, hs)
        .transpose(0, 2, 1, 3, 4)
        .reshape(head_count, owners, owned * SLOTS, hs)
    )
    returned = lax.all_to_all(attended, "seq", split_axis=1, concat_axis=1, tiled=True)
    key_sums = jnp.einsum(
        "hck,hckd->hcd", filled.astype(jnp.bfloat16), key_block, preferred_element_type=jnp.float32
    )
    counts = jnp.sum(filled, axis=2).astype(jnp.float32)
    gathered = returned.reshape(head_count, clusters * SLOTS, hs)
    mine = jax.vmap(lambda table, where: table[where])(gathered, placed)
    context = mine.transpose(1, 0, 2).reshape(local_rows, head_count * hs)
    updated = 0.25 * centroids + 0.75 * key_sums / jnp.maximum(counts, 1.0)[:, :, None]
    return (context, updated)


def attend_kernel(hs, block, qkv_ref, id_col_ref, id_row_ref, out_ref):
    rows = qkv_ref.shape[0]
    scale = hs ** (-0.5)
    for start in range(0, rows, block):
        stop = start + block
        queries = qkv_ref[start:stop, :hs]
        keys = qkv_ref[:stop, hs : 2 * hs]
        values = qkv_ref[:stop, 2 * hs :]
        scores = lax.dot_general(
            queries, keys, (((1,), (1,)), ((), ())), preferred_element_type=jnp.float32
        )
        allowed = id_col_ref[start:stop, :] == id_row_ref[:, :stop]
        row_at = lax.broadcasted_iota(jnp.int32, (block, stop), 0) + start
        col_at = lax.broadcasted_iota(jnp.int32, (block, stop), 1)
        scores = jnp.where(allowed & (col_at <= row_at), scores * scale, -1e30)
        raised = jnp.exp(scores - jnp.max(scores, axis=1, keepdims=True))
        total = jnp.sum(raised, axis=1, keepdims=True)
        mixed = jnp.dot(raised.astype(jnp.bfloat16), values, preferred_element_type=jnp.float32)
        out_ref[start:stop, :] = (mixed / total).astype(out_ref.dtype)


def attend(qkv, id_col, id_row, hs):
    rows = qkv.shape[0]
    block = min(256, rows)
    return pl.pallas_call(
        lambda *refs: attend_kernel(hs, block, *refs),
        out_shape=jax.ShapeDtypeStruct((rows, hs), jnp.bfloat16),
        cost_estimate=pl.CostEstimate(
            flops=2 * rows * rows * hs, bytes_accessed=rows * hs * 8, transcendentals=rows * rows
        ),
        name="attend",
    )(qkv, id_col, id_row)


def means_kernel(hs, qkv_ref, id_row_ref, out_ref):
    clusters, rows = out_ref.shape[0], qkv_ref.shape[0]
    label = lax.broadcasted_iota(jnp.int32, (clusters, rows), 0)
    onehot = (label == id_row_ref[...]).astype(jnp.float32)
    counts = jnp.sum(onehot, axis=1, keepdims=True)
    sums = jnp.dot(
        onehot.astype(jnp.bfloat16), qkv_ref[:, hs : 2 * hs], preferred_element_type=jnp.float32
    )
    out_ref[...] = 0.75 * sums / jnp.maximum(counts, 1.0)


def means(qkv, id_row, clusters, hs):
    rows = qkv.shape[0]
    return pl.pallas_call(
        lambda *refs: means_kernel(hs, *refs),
        out_shape=jax.ShapeDtypeStruct((clusters, hs), jnp.float32),
        cost_estimate=pl.CostEstimate(
            flops=2 * rows * clusters * hs, bytes_accessed=rows * hs * 2, transcendentals=0
        ),
        name="means",
    )(qkv, id_row)


def arrivals(size):
    table = []
    for z in range(size):
        order = []
        for step in range(1, size):
            if step <= z:
                order.append((0, step))
            if step <= size - 1 - z:
                order.append((1, step))
        table.append(order)
    return table


def by_head(tokens, proj_weight, cluster_ids, centroids):
    seq, heads, groups = (lax.axis_size(a) for a in ("seq", "head", "groups"))
    z, h, y = (lax.axis_index(a) for a in ("seq", "head", "groups"))
    core, x, xs = h % CORES, h // CORES, heads // CORES
    local_rows, depth = tokens.shape
    hs = centroids.shape[2]
    clusters = centroids.shape[1] * seq
    slice_depth = proj_weight.shape[1]
    half = slice_depth // CORES
    part = half // groups
    rows = local_rows // xs
    width = 3 * hs

    def swap_core(v):
        return lax.ppermute(v, "head", [(i, i ^ 1) for i in range(heads)])

    def shift_x(v, d):
        pairs = [(i, (i // CORES + d) % xs * CORES + i % CORES) for i in range(heads)]
        return lax.ppermute(v, "head", pairs)

    def shift_y(v, d):
        return lax.ppermute(v, "groups", [(i, (i + d) % groups) for i in range(groups)])

    def shift_z(v, d):
        return lax.ppermute(v, "seq", [(i, (i + d) % seq) for i in range(seq)])

    def line_z(v, d):
        return lax.ppermute(v, "seq", [(i, i + d) for i in range(seq) if 0 <= i + d < seq])

    own = tokens.reshape(local_rows, seq, CORES, half)
    own = lax.dynamic_index_in_dim(own, core, 2, keepdims=False).reshape(local_rows, seq * half)
    mine = lax.dynamic_slice_in_dim(own, x * rows, rows, 0)

    weight = proj_weight.reshape(3, CORES, groups, part, seq, hs)

    def weight_of(c):
        w = lax.dynamic_index_in_dim(weight, c, 1, keepdims=False)
        w = lax.dynamic_index_in_dim(w, y, 1, keepdims=False)
        return w.transpose(2, 1, 0, 3).reshape(seq, part, width)

    kept = weight_of(core)
    given = swap_core(weight_of(1 - core))
    both = jnp.concatenate([kept, given], axis=2)
    matrix = jnp.zeros((seq, groups, part, CORES * width), jnp.bfloat16)
    zero = jnp.int32(0)
    for d in range(seq):
        piece = lax.dynamic_index_in_dim(both, (z + d) % seq, 0, keepdims=False)
        if d:
            piece = shift_z(piece, d)
        for g in range(groups):
            moved = shift_y(piece, g) if g else piece
            at = ((z - d) % seq, (y - g) % groups, zero, zero)
            matrix = lax.dynamic_update_slice(matrix, moved[None, None], at)
    matrix = matrix.reshape(seq * half, CORES * width)

    right, left = [mine], [mine]
    for step in range(1, seq):
        right.append(line_z(right[-1], 1))
        left.append(line_z(left[-1], -1))
    table = arrivals(seq)

    member = lax.all_to_all(cluster_ids[:, :, 0], "seq", split_axis=0, concat_axis=0, tiled=True)

    def project(block):
        return jnp.dot(block, matrix, preferred_element_type=jnp.float32)

    def finish(full):
        theirs = swap_core(full[:, width:])
        return (full[:, :width] + theirs).astype(jnp.bfloat16)

    qkv = jnp.zeros((seq, xs, rows, width), jnp.bfloat16)
    qkv = lax.dynamic_update_slice(
        qkv, finish(project(own)).reshape(1, xs, rows, width), (z, zero, zero, zero)
    )
    for k in range(seq - 1):
        picks = {}
        for at in range(seq):
            picks.setdefault(table[at][k], []).append(at)
        block, source = None, None
        for (direction, step), where in picks.items():
            value = (right, left)[direction][step]
            origin = z + (step if direction else -step)
            if block is None:
                block, source = value, origin
            else:
                chosen = sum((z == at).astype(jnp.int32) for at in where) > 0
                block = jnp.where(chosen, value, block)
                source = jnp.where(chosen, origin, source)
        pieces = [block] + [shift_x(block, d) for d in range(1, xs)]
        full = jnp.concatenate([project(p) for p in pieces], axis=0)
        done = finish(full)
        for d in range(xs):
            at = (source, (x - d) % xs, zero, zero)
            qkv = lax.dynamic_update_slice(qkv, done[d * rows : (d + 1) * rows][None, None], at)
    qkv = qkv.reshape(seq * local_rows, width)

    id_row = member.reshape(1, seq * local_rows)
    id_col = member.reshape(seq * local_rows, 1)
    moved = means(qkv, id_row, clusters, hs)
    moved = lax.all_to_all(
        moved.reshape(seq, clusters // seq, hs), "seq", split_axis=0, concat_axis=0, tiled=True
    )
    updated = 0.25 * centroids + moved
    mixed = attend(qkv, id_col, id_row, hs).reshape(seq, local_rows, hs)
    mixed = lax.all_to_all(mixed, "seq", split_axis=0, concat_axis=0, tiled=True)
    context = mixed.transpose(1, 0, 2).reshape(local_rows, seq * hs)
    return (context, updated)


def local(tokens, proj_weight, cluster_ids, centroids):
    seq, heads = lax.axis_size("seq"), lax.axis_size("head")
    if cluster_ids.shape[0] == seq and heads % CORES == 0:
        return by_head(tokens, proj_weight, cluster_ids, centroids)
    return routed(tokens, proj_weight, cluster_ids, centroids)


def solution(mesh):
    return jax.shard_map(
        local,
        mesh=mesh,
        in_specs=(
            P(("groups", "seq"), None),
            P(None, "seq", "head"),
            P("head", ("groups", "seq"), None),
            P(("groups", "head"), "seq", None),
        ),
        out_specs=(P(("groups", "seq"), "head"), P(("groups", "head"), "seq", None)),
        check_vma=False,
    )
```

```python
import jax
import jax.numpy as jnp
from jax import lax
from jax.experimental import pallas as pl
from jax.experimental.pallas import tpu as pltpu
from jax.sharding import PartitionSpec as P

SLOTS = 4
CORES = 2


def routed(tokens, proj_weight, cluster_ids, centroids):
    owners = lax.axis_size("seq")
    local_rows = tokens.shape[0]
    hs = centroids.shape[2]
    clusters = centroids.shape[1] * owners
    columns = proj_weight.shape[2]
    head_count = columns // hs
    owned = clusters // owners
    capacity = owners * SLOTS
    score_scale = hs ** (-0.5)
    projected = jnp.einsum(
        "td,pdc->ptc",
        tokens,
        lax.all_gather(proj_weight, "seq", axis=1, tiled=True),
        preferred_element_type=jnp.float32,
    ).astype(jnp.bfloat16)
    per_head = projected.reshape(3, local_rows, head_count, hs).transpose(2, 1, 0, 3)
    packed = per_head.reshape(head_count, local_rows, 3 * hs)
    member = cluster_ids[:, :, 0]
    labels = jnp.arange(clusters, dtype=jnp.int32)
    onehot = (member[:, :, None] == labels[None, None, :]).astype(jnp.bfloat16)
    ordinal_rows = jnp.arange(local_rows, dtype=jnp.int32)
    earlier = (ordinal_rows[None, :] < ordinal_rows[:, None]).astype(jnp.bfloat16)
    before = jnp.einsum("ts,hsc->htc", earlier, onehot, preferred_element_type=jnp.float32)
    ranking = jnp.take_along_axis(before, member[:, :, None], axis=2)[:, :, 0].astype(jnp.int32)
    placed = member * SLOTS + ranking
    head_index = jnp.arange(head_count, dtype=jnp.int32)[:, None]
    outbox = (
        jnp.zeros((head_count, clusters * SLOTS, 3 * hs), jnp.bfloat16)
        .at[head_index, placed]
        .set(packed)
    )
    outbox = outbox.reshape(head_count, owners, owned * SLOTS, 3 * hs)
    local_counts = jnp.sum(onehot, axis=1, dtype=jnp.float32)
    tallies = local_counts.astype(jnp.int32).reshape(head_count, owners, owned)
    blocks = lax.all_to_all(outbox, "seq", split_axis=1, concat_axis=1, tiled=True)
    arrived = lax.all_to_all(tallies, "seq", split_axis=1, concat_axis=1, tiled=True)
    arranged = (
        blocks.reshape(head_count, owners, owned, SLOTS, 3 * hs)
        .transpose(0, 2, 1, 3, 4)
        .reshape(head_count, owned, capacity, 3 * hs)
    )
    filled = jnp.arange(SLOTS, dtype=jnp.int32)[None, None, None, :] < arrived[:, :, :, None]
    filled = filled.transpose(0, 2, 1, 3).reshape(head_count, owned, capacity)
    queries = arranged[:, :, :, :hs]
    key_block = arranged[:, :, :, hs : 2 * hs]
    value_block = arranged[:, :, :, 2 * hs :]
    scores = (
        jnp.einsum("hcqd,hckd->hcqk", queries, key_block, preferred_element_type=jnp.float32)
        * score_scale
    )
    ordinal = jnp.arange(capacity, dtype=jnp.int32)
    causal = ordinal[None, None, None, :] <= ordinal[None, None, :, None]
    itself = ordinal[None, None, None, :] == ordinal[None, None, :, None]
    allowed = filled[:, :, None, :] & causal | itself
    scores = jnp.where(allowed, scores, -1e30)
    row_max = jnp.max(scores, axis=3, keepdims=True)
    raised = jnp.exp(scores - row_max)
    weights = (raised / jnp.sum(raised, axis=3, keepdims=True)).astype(jnp.bfloat16)
    attended = jnp.einsum(
        "hcqk,hckd->hcqd", weights, value_block, preferred_element_type=jnp.float32
    ).astype(jnp.bfloat16)
    attended = (
        attended.reshape(head_count, owned, owners, SLOTS, hs)
        .transpose(0, 2, 1, 3, 4)
        .reshape(head_count, owners, owned * SLOTS, hs)
    )
    returned = lax.all_to_all(attended, "seq", split_axis=1, concat_axis=1, tiled=True)
    key_sums = jnp.einsum(
        "hck,hckd->hcd", filled.astype(jnp.bfloat16), key_block, preferred_element_type=jnp.float32
    )
    counts = jnp.sum(filled, axis=2).astype(jnp.float32)
    gathered = returned.reshape(head_count, clusters * SLOTS, hs)
    mine = jax.vmap(lambda table, where: table[where])(gathered, placed)
    context = mine.transpose(1, 0, 2).reshape(local_rows, head_count * hs)
    updated = 0.25 * centroids + 0.75 * key_sums / jnp.maximum(counts, 1.0)[:, :, None]
    return (context, updated)


def attend_kernel(hs, local_rows, qkv_ref, id_col_ref, id_row_ref, out_ref):
    rows = qkv_ref.shape[0]
    owned = out_ref.shape[1] - local_rows
    block = min(256, local_rows)
    scale = hs ** (-0.5)
    for start in range(0, rows, block):
        stop = start + block
        queries = qkv_ref[start:stop, :hs]
        keys = qkv_ref[:stop, hs : 2 * hs]
        values = qkv_ref[:stop, 2 * hs :]
        scores = lax.dot_general(
            queries, keys, (((1,), (1,)), ((), ())), preferred_element_type=jnp.float32
        )
        allowed = id_col_ref[start:stop, :] == id_row_ref[:, :stop]
        row_at = lax.broadcasted_iota(jnp.int32, (block, stop), 0) + start
        col_at = lax.broadcasted_iota(jnp.int32, (block, stop), 1)
        scores = jnp.where(allowed & (col_at <= row_at), scores * scale, -1e30)
        raised = jnp.exp(scores - jnp.max(scores, axis=1, keepdims=True))
        total = jnp.sum(raised, axis=1, keepdims=True)
        mixed = jnp.dot(raised.astype(jnp.bfloat16), values, preferred_element_type=jnp.float32)
        at = start % local_rows
        out_ref[start // local_rows, at : at + block, :] = (mixed / total).astype(out_ref.dtype)
    keys = qkv_ref[:, hs : 2 * hs]
    for owner in range(out_ref.shape[0]):
        label = lax.broadcasted_iota(jnp.int32, (owned, rows), 0) + owner * owned
        onehot = (label == id_row_ref[...]).astype(jnp.float32)
        counts = jnp.sum(onehot, axis=1, keepdims=True)
        sums = jnp.dot(onehot.astype(jnp.bfloat16), keys, preferred_element_type=jnp.float32)
        mean = 0.75 * sums / jnp.maximum(counts, 1.0)
        out_ref[owner, local_rows:, :] = mean.astype(out_ref.dtype)


def attend(qkv, id_col, id_row, seq, owned, hs):
    rows = qkv.shape[0]
    local_rows = rows // seq
    return pl.pallas_call(
        lambda *refs: attend_kernel(hs, local_rows, *refs),
        out_shape=jax.ShapeDtypeStruct((seq, local_rows + owned, hs), jnp.bfloat16),
        cost_estimate=pl.CostEstimate(
            flops=2 * rows * rows * hs, bytes_accessed=rows * hs * 8, transcendentals=rows * rows
        ),
        name="attend",
    )(qkv, id_col, id_row)


def arrivals(size):
    table = []
    for z in range(size):
        order = []
        for step in range(1, size):
            if step <= z:
                order.append((0, step))
            if step <= size - 1 - z:
                order.append((1, step))
        table.append(order)
    return table


def copy_kernel(place, in_ref, out_ref):
    out_ref[...] = in_ref[...]


def take(tokens, place, rows, width, stride):
    depth = tokens.shape[1]
    runs, per = depth // stride, stride // width
    return pl.pallas_call(
        copy_kernel,
        out_shape=jax.ShapeDtypeStruct((rows, runs * width), tokens.dtype),
        grid_spec=pltpu.PrefetchScalarGridSpec(
            num_scalar_prefetch=1,
            grid=(runs,),
            in_specs=[pl.BlockSpec((rows, width), lambda i, p: (p[0], i * per + p[1]))],
            out_specs=pl.BlockSpec((rows, width), lambda i, p: (0, i)),
        ),
        cost_estimate=pl.CostEstimate(
            flops=0, bytes_accessed=4 * rows * runs * width, transcendentals=0
        ),
        name="take",
    )(place, tokens)


def unpack_kernel(hs, place, in_ref, out_ref):
    for head in range(out_ref.shape[0]):
        for which in range(3):
            out_ref[head, :, which * hs : (which + 1) * hs] = in_ref[
                which, :, head * hs : (head + 1) * hs
            ]


def unpack(weight, place, rows, hs):
    heads = weight.shape[2] // hs
    steps = 2 if rows % 32 == 0 else 1
    return pl.pallas_call(
        lambda *refs: unpack_kernel(hs, *refs),
        out_shape=jax.ShapeDtypeStruct((heads, rows, 3 * hs), weight.dtype),
        grid_spec=pltpu.PrefetchScalarGridSpec(
            num_scalar_prefetch=1,
            grid=(steps,),
            in_specs=[
                pl.BlockSpec(
                    (3, rows // steps, heads * hs), lambda i, p: (0, p[0] * steps + i, 0)
                )
            ],
            out_specs=pl.BlockSpec((heads, rows // steps, 3 * hs), lambda i, p: (0, i, 0)),
        ),
        cost_estimate=pl.CostEstimate(
            flops=0, bytes_accessed=12 * rows * heads * hs, transcendentals=0
        ),
        name="unpack",
    )(place, weight)


def by_head(tokens, proj_weight, cluster_ids, centroids):
    seq, heads, groups = (lax.axis_size(a) for a in ("seq", "head", "groups"))
    z, h, y = (lax.axis_index(a) for a in ("seq", "head", "groups"))
    core, x, xs = h % CORES, h // CORES, heads // CORES
    local_rows, _ = tokens.shape
    hs = centroids.shape[2]
    slice_depth = proj_weight.shape[1]
    half = slice_depth // CORES
    part = half // groups
    rows = local_rows // xs
    width = 3 * hs
    zero = jnp.int32(0)
    tie = lax.optimization_barrier

    def swap_core(v):
        return lax.ppermute(v, "head", [(i, i ^ 1) for i in range(heads)])

    def shift_x(v, d):
        pairs = [(i, (i // CORES + d) % xs * CORES + i % CORES) for i in range(heads)]
        return lax.ppermute(v, "head", pairs)

    def shift_y(v, d):
        return lax.ppermute(v, "groups", [(i, (i + d) % groups) for i in range(groups)])

    def shift_z(v, d):
        return lax.ppermute(v, "seq", [(i, (i + d) % seq) for i in range(seq)])

    def line_z(v, d):
        pairs = [(i, i + d) for i in range(seq) if 0 <= i + d < seq]
        return lax.ppermute(v, "seq", pairs)

    mine = take(tokens, jnp.stack([x, core]).astype(jnp.int32), rows, half, slice_depth)
    right, left = [(mine,)], [(mine,)]
    right.append((line_z(mine, 1),))
    left.append((line_z(mine, -1),))

    mine, weight, tokens = tie((mine, proj_weight, tokens))
    given = unpack(weight, jnp.stack([(1 - core) * groups + y]).astype(jnp.int32), part, hs)
    given = swap_core(given)
    kept = unpack(weight, jnp.stack([core * groups + y]).astype(jnp.int32), part, hs)
    own = take(tokens, jnp.stack([zero, core]).astype(jnp.int32), local_rows, half, slice_depth)
    both = jnp.concatenate([kept, given], axis=2)
    member = lax.all_to_all(cluster_ids[:, :, 0], "seq", split_axis=0, concat_axis=0, tiled=True)
    id_row = member.reshape(1, seq * local_rows)
    id_col = member.reshape(seq * local_rows, 1)

    right[1], left[1], both = tie((right[1], left[1], both))
    for step in range(2, seq):
        chunks = 2 if step == seq - 1 and rows % 32 == 0 else 1
        for way, d in ((right, 1), (left, -1)):
            parts = [p for v in way[-1] for p in jnp.split(v, chunks // len(way[-1]), axis=0)]
            way.append(tuple(line_z(p, d) for p in parts))
    pieces = []
    for d in sorted(range(seq), key=lambda d: min(d, seq - d)):
        piece = lax.dynamic_index_in_dim(both, (z + d) % seq, 0, keepdims=False)
        pieces.append((d, shift_z(piece, d) if d else piece))
    matrix = jnp.zeros((seq, groups, part, CORES * width), jnp.bfloat16)
    for d, piece in pieces:
        for g in range(groups):
            moved = shift_y(piece, g) if g else piece
            at = ((z - d) % seq, (y - g) % groups, zero, zero)
            matrix = lax.dynamic_update_slice(matrix, moved[None, None], at)
    matrix = matrix.reshape(seq * half, CORES * width)

    table = arrivals(seq)

    def project(block):
        return jnp.dot(block, matrix, preferred_element_type=jnp.float32)

    def finish(full):
        theirs = swap_core(full[:, width:])
        return (full[:, :width] + theirs).astype(jnp.bfloat16)

    qkv = jnp.zeros((seq, local_rows, width), jnp.bfloat16)
    qkv = lax.dynamic_update_slice(qkv, finish(project(own))[None], (z, zero, zero))
    last = None
    for k in range(seq - 1):
        picks = {}
        for at in range(seq):
            picks.setdefault(table[at][k], []).append(at)
        chunks = max(len((right, left)[a][b]) for a, b in picks)
        size = rows // chunks
        for chunk in range(chunks):
            block, source = None, None
            values = []
            for direction, step in picks:
                value = (right, left)[direction][step]
                if len(value) == chunks:
                    values.append(value[chunk])
                else:
                    values.append(value[0][chunk * size : (chunk + 1) * size])
            if last is not None:
                values, last = tie((values, last))
            for value, ((direction, step), where) in zip(values, picks.items()):
                origin = z + (step if direction else -step)
                if block is None:
                    block, source = value, origin
                else:
                    chosen = sum((z == at).astype(jnp.int32) for at in where) > 0
                    block = jnp.where(chosen, value, block)
                    source = jnp.where(chosen, origin, source)
            parts = [block] + [shift_x(block, d) for d in range(1, xs)]
            last = block
            done = finish(jnp.concatenate([project(p) for p in parts], axis=0))
            for d in range(xs):
                at = (source, (x - d) % xs * rows + chunk * size, zero)
                qkv = lax.dynamic_update_slice(qkv, done[d * size : (d + 1) * size][None], at)
    qkv = qkv.reshape(seq * local_rows, width)

    owned = centroids.shape[1]
    mixed = attend(qkv, id_col, id_row, seq, owned, hs)
    mixed = lax.all_to_all(mixed, "seq", split_axis=0, concat_axis=0, tiled=True)
    context = mixed[:, :local_rows].transpose(1, 0, 2).reshape(local_rows, seq * hs)
    updated = 0.25 * centroids + mixed[:, local_rows:].astype(jnp.float32)
    return (context, updated)


def local(tokens, proj_weight, cluster_ids, centroids):
    seq, heads = lax.axis_size("seq"), lax.axis_size("head")
    if cluster_ids.shape[0] == seq and heads % CORES == 0:
        return by_head(tokens, proj_weight, cluster_ids, centroids)
    return routed(tokens, proj_weight, cluster_ids, centroids)


def solution(mesh):
    return jax.shard_map(
        local,
        mesh=mesh,
        in_specs=(
            P(("groups", "seq"), None),
            P(None, "seq", "head"),
            P("head", ("groups", "seq"), None),
            P(("groups", "head"), "seq", None),
        ),
        out_specs=(P(("groups", "seq"), "head"), P(("groups", "head"), "seq", None)),
        check_vma=False,
    )
```

```python
import jax
import jax.numpy as jnp
from jax import lax
from jax.experimental import pallas as pl
from jax.experimental.pallas import tpu as pltpu
from jax.sharding import PartitionSpec as P

SLOTS = 4
CORES = 2
SMALL_VMEM = 16 << 20


def routed(tokens, proj_weight, cluster_ids, centroids):
    owners = lax.axis_size("seq")
    local_rows = tokens.shape[0]
    hs = centroids.shape[2]
    clusters = centroids.shape[1] * owners
    columns = proj_weight.shape[2]
    head_count = columns // hs
    owned = clusters // owners
    capacity = owners * SLOTS
    score_scale = hs ** (-0.5)
    projected = jnp.einsum(
        "td,pdc->ptc",
        tokens,
        lax.all_gather(proj_weight, "seq", axis=1, tiled=True),
        preferred_element_type=jnp.float32,
    ).astype(jnp.bfloat16)
    per_head = projected.reshape(3, local_rows, head_count, hs).transpose(2, 1, 0, 3)
    packed = per_head.reshape(head_count, local_rows, 3 * hs)
    member = cluster_ids[:, :, 0]
    labels = jnp.arange(clusters, dtype=jnp.int32)
    onehot = (member[:, :, None] == labels[None, None, :]).astype(jnp.bfloat16)
    ordinal_rows = jnp.arange(local_rows, dtype=jnp.int32)
    earlier = (ordinal_rows[None, :] < ordinal_rows[:, None]).astype(jnp.bfloat16)
    before = jnp.einsum("ts,hsc->htc", earlier, onehot, preferred_element_type=jnp.float32)
    ranking = jnp.take_along_axis(before, member[:, :, None], axis=2)[:, :, 0].astype(jnp.int32)
    placed = member * SLOTS + ranking
    head_index = jnp.arange(head_count, dtype=jnp.int32)[:, None]
    outbox = (
        jnp.zeros((head_count, clusters * SLOTS, 3 * hs), jnp.bfloat16)
        .at[head_index, placed]
        .set(packed)
    )
    outbox = outbox.reshape(head_count, owners, owned * SLOTS, 3 * hs)
    local_counts = jnp.sum(onehot, axis=1, dtype=jnp.float32)
    tallies = local_counts.astype(jnp.int32).reshape(head_count, owners, owned)
    blocks = lax.all_to_all(outbox, "seq", split_axis=1, concat_axis=1, tiled=True)
    arrived = lax.all_to_all(tallies, "seq", split_axis=1, concat_axis=1, tiled=True)
    arranged = (
        blocks.reshape(head_count, owners, owned, SLOTS, 3 * hs)
        .transpose(0, 2, 1, 3, 4)
        .reshape(head_count, owned, capacity, 3 * hs)
    )
    filled = jnp.arange(SLOTS, dtype=jnp.int32)[None, None, None, :] < arrived[:, :, :, None]
    filled = filled.transpose(0, 2, 1, 3).reshape(head_count, owned, capacity)
    queries = arranged[:, :, :, :hs]
    key_block = arranged[:, :, :, hs : 2 * hs]
    value_block = arranged[:, :, :, 2 * hs :]
    scores = (
        jnp.einsum("hcqd,hckd->hcqk", queries, key_block, preferred_element_type=jnp.float32)
        * score_scale
    )
    ordinal = jnp.arange(capacity, dtype=jnp.int32)
    causal = ordinal[None, None, None, :] <= ordinal[None, None, :, None]
    itself = ordinal[None, None, None, :] == ordinal[None, None, :, None]
    allowed = filled[:, :, None, :] & causal | itself
    scores = jnp.where(allowed, scores, -1e30)
    row_max = jnp.max(scores, axis=3, keepdims=True)
    raised = jnp.exp(scores - row_max)
    weights = (raised / jnp.sum(raised, axis=3, keepdims=True)).astype(jnp.bfloat16)
    attended = jnp.einsum(
        "hcqk,hckd->hcqd", weights, value_block, preferred_element_type=jnp.float32
    ).astype(jnp.bfloat16)
    attended = (
        attended.reshape(head_count, owned, owners, SLOTS, hs)
        .transpose(0, 2, 1, 3, 4)
        .reshape(head_count, owners, owned * SLOTS, hs)
    )
    returned = lax.all_to_all(attended, "seq", split_axis=1, concat_axis=1, tiled=True)
    key_sums = jnp.einsum(
        "hck,hckd->hcd", filled.astype(jnp.bfloat16), key_block, preferred_element_type=jnp.float32
    )
    counts = jnp.sum(filled, axis=2).astype(jnp.float32)
    gathered = returned.reshape(head_count, clusters * SLOTS, hs)
    mine = jax.vmap(lambda table, where: table[where])(gathered, placed)
    context = mine.transpose(1, 0, 2).reshape(local_rows, head_count * hs)
    updated = 0.25 * centroids + 0.75 * key_sums / jnp.maximum(counts, 1.0)[:, :, None]
    return (context, updated)


def attend_kernel(hs, local_rows, place, qkv_ref, id_col_ref, id_row_ref, out_ref):
    rows = qkv_ref.shape[0]
    owned = out_ref.shape[0] - local_rows
    block = min(256, local_rows)
    scale = hs ** (-0.5)
    at = place[0] * local_rows

    for first in range(0, local_rows, block):
        here = pl.multiple_of(at + first, block)
        queries = qkv_ref[pl.ds(here, block), :hs]
        ids = id_col_ref[pl.ds(here, block), :]

        def scores_of(start, size):
            keys = qkv_ref[pl.ds(start, size), hs : 2 * hs]
            scores = lax.dot_general(
                queries, keys, (((1,), (1,)), ((), ())), preferred_element_type=jnp.float32
            )
            return scores * scale, ids == id_row_ref[:, pl.ds(start, size)]

        def mix(raised, start, size):
            values = qkv_ref[pl.ds(start, size), 2 * hs :]
            return jnp.dot(raised.astype(jnp.bfloat16), values, preferred_element_type=jnp.float32)

        size = first + block
        base = pl.multiple_of(at, local_rows)
        scores, allowed = scores_of(base, size)
        row_at = lax.broadcasted_iota(jnp.int32, (block, size), 0) + first
        col_at = lax.broadcasted_iota(jnp.int32, (block, size), 1)
        scores = jnp.where(allowed & (col_at <= row_at), scores, -1e30)
        peak = jnp.max(scores, axis=1, keepdims=True)
        raised = jnp.exp(scores - peak)
        total = jnp.sum(raised, axis=1, keepdims=True)
        mixed = mix(raised, base, size)

        def earlier(j, carry):
            peak, total, mixed = carry
            start = pl.multiple_of(j * local_rows, local_rows)
            scores, allowed = scores_of(start, local_rows)
            scores = jnp.where(allowed, scores, -1e30)
            higher = jnp.maximum(peak, jnp.max(scores, axis=1, keepdims=True))
            kept = jnp.exp(peak - higher)
            raised = jnp.exp(scores - higher)
            total = total * kept + jnp.sum(raised, axis=1, keepdims=True)
            return higher, total, mixed * kept + mix(raised, start, local_rows)

        _, total, mixed = lax.fori_loop(0, place[0], earlier, (peak, total, mixed))
        out_ref[first : first + block, :] = (mixed / total).astype(out_ref.dtype)
    label = lax.broadcasted_iota(jnp.int32, (owned, rows), 0) + place[0] * owned
    onehot = (label == id_row_ref[...]).astype(jnp.float32)
    counts = jnp.sum(onehot, axis=1, keepdims=True)
    keys = qkv_ref[:, hs : 2 * hs]
    sums = jnp.dot(onehot.astype(jnp.bfloat16), keys, preferred_element_type=jnp.float32)
    mean = 0.75 * sums / jnp.maximum(counts, 1.0)
    out_ref[local_rows:, :] = mean.astype(out_ref.dtype)


def whole(shape):
    return pl.BlockSpec(shape, lambda i, p: (0,) * len(shape))


def attend(place, qkv, id_col, id_row, seq, owned, hs):
    rows = qkv.shape[0]
    shape = (rows // seq + owned, hs)
    return pl.pallas_call(
        lambda *refs: attend_kernel(hs, rows // seq, *refs),
        out_shape=jax.ShapeDtypeStruct(shape, jnp.bfloat16),
        grid_spec=pltpu.PrefetchScalarGridSpec(
            num_scalar_prefetch=1,
            grid=(1,),
            in_specs=[whole(v.shape) for v in (qkv, id_col, id_row)],
            out_specs=whole(shape),
        ),
        compiler_params=pltpu.CompilerParams(vmem_limit_bytes=SMALL_VMEM),
        cost_estimate=pl.CostEstimate(
            flops=rows * rows * hs, bytes_accessed=rows * hs * 8, transcendentals=rows * rows // 4
        ),
        name="attend",
    )(place, qkv, id_col, id_row)


def collect_kernel(hs, local_rows, place, *refs):
    *pieces, centroid_ref, context_ref, updated_ref = refs
    for d, piece in enumerate(pieces):
        source = place[d]
        columns = pl.ds(pl.multiple_of(source * hs, hs), hs)
        context_ref[:, columns] = piece[:local_rows, :]
        mean = piece[local_rows:, :].astype(jnp.float32)
        updated_ref[source] = 0.25 * centroid_ref[source] + mean


def collect(place, pieces, centroids, local_rows):
    hs = centroids.shape[2]
    shape = (local_rows, len(pieces) * hs)
    return pl.pallas_call(
        lambda *refs: collect_kernel(hs, local_rows, *refs),
        out_shape=(
            jax.ShapeDtypeStruct(shape, jnp.bfloat16),
            jax.ShapeDtypeStruct(centroids.shape, jnp.float32),
        ),
        grid_spec=pltpu.PrefetchScalarGridSpec(
            num_scalar_prefetch=1,
            grid=(1,),
            in_specs=[whole(v.shape) for v in (*pieces, centroids)],
            out_specs=[whole(shape), whole(centroids.shape)],
        ),
        compiler_params=pltpu.CompilerParams(vmem_limit_bytes=SMALL_VMEM),
        cost_estimate=pl.CostEstimate(flops=0, bytes_accessed=1 << 20, transcendentals=0),
        name="collect",
    )(place, *pieces, centroids)


def choose(index, values):
    chosen = values[0]
    for i, value in enumerate(values[1:], 1):
        chosen = jnp.where(index == i, value, chosen)
    return chosen


def project_kernel(counts, spots, *refs):
    weights, tokens = refs[: counts[0]], refs[counts[0] : sum(counts)]
    kept_ref, sent_ref, matrix, held, weight_sem, token_sem = refs[sum(counts) :]
    step = pl.program_id(0)
    block, width = kept_ref.shape
    part = weights[0].shape[0]
    copies, row = {}, 0
    for i, ref in enumerate(tokens):
        to = held.at[row : row + ref.shape[0], :]
        copy = pltpu.make_async_copy(ref, to, token_sem.at[i])
        copies.setdefault(row // block, []).append(copy)
        row += ref.shape[0]

    @pl.when(step == 0)
    def _():
        loads = []
        for i, ref in enumerate(weights):
            to = matrix.at[pl.ds(pl.multiple_of(spots[i] * part, part), part), :]
            loads.append(pltpu.make_async_copy(ref, to, weight_sem.at[i]))
        loads += copies[0]
        for copy in loads:
            copy.start()
        for copy in loads:
            copy.wait()
        for at, group in copies.items():
            for copy in group if at else []:
                copy.start()

    for at, group in copies.items():

        @pl.when(step == at)
        def _(group=group):
            for copy in group if at else []:
                copy.wait()

    left = held[pl.ds(pl.multiple_of(step * block, block), block), :]
    full = jnp.dot(left, matrix[...], preferred_element_type=jnp.float32)
    kept_ref[...] = full[:, :width]
    sent_ref[...] = full[:, width:].astype(sent_ref.dtype)


def project(spots, weights, tokens, block):
    depth = weights[0].shape[0] * len(weights)
    width = weights[0].shape[1] // CORES
    total = sum(v.shape[0] for v in tokens)
    counts = len(weights), len(tokens)
    return pl.pallas_call(
        lambda *refs: project_kernel(counts, *refs),
        out_shape=(
            jax.ShapeDtypeStruct((total, width), jnp.float32),
            jax.ShapeDtypeStruct((total, width), jnp.bfloat16),
        ),
        grid_spec=pltpu.PrefetchScalarGridSpec(
            num_scalar_prefetch=1,
            grid=(total // block,),
            in_specs=[pl.BlockSpec(memory_space=pl.ANY)] * sum(counts),
            out_specs=[pl.BlockSpec((block, width), lambda i, p: (i, 0))] * 2,
            scratch_shapes=[
                pltpu.VMEM((depth, CORES * width), jnp.bfloat16),
                pltpu.VMEM((total, depth), jnp.bfloat16),
                pltpu.SemaphoreType.DMA((counts[0],)),
                pltpu.SemaphoreType.DMA((counts[1],)),
            ],
        ),
        compiler_params=pltpu.CompilerParams(dimension_semantics=("arbitrary",)),
        cost_estimate=pl.CostEstimate(
            flops=2 * total * depth * CORES * width,
            bytes_accessed=2 * depth * (total + CORES * width) + 8 * total * width,
            transcendentals=0,
        ),
        name="project",
    )(spots, *weights, *tokens)


def merge_kernel(block, place, kept_hbm, theirs_hbm, out_ref, kept, theirs, sems):
    count = kept.shape[0] // block
    copies = []
    for i in range(count):
        down = pl.ds(i * block, block)
        pair = (
            pltpu.make_async_copy(kept_hbm.at[down], kept.at[down], sems.at[0, i]),
            pltpu.make_async_copy(theirs_hbm.at[down], theirs.at[down], sems.at[1, i]),
        )
        for copy in pair:
            copy.start()
        copies.append(pair)
    for i, pair in enumerate(copies):
        for copy in pair:
            copy.wait()
        here = slice(i * block, (i + 1) * block)
        both = kept[here, :] + theirs[here, :].astype(jnp.float32)
        to = pl.ds(pl.multiple_of(place[i] * block, block), block)
        out_ref[to, :] = both.astype(out_ref.dtype)


def merge(at, kept, theirs, total, block):
    rows, width = kept.shape
    anywhere = pl.BlockSpec(memory_space=pl.ANY)
    return pl.pallas_call(
        lambda *refs: merge_kernel(block, *refs),
        out_shape=jax.ShapeDtypeStruct((total, width), jnp.bfloat16),
        grid_spec=pltpu.PrefetchScalarGridSpec(
            num_scalar_prefetch=1,
            grid=(1,),
            in_specs=[anywhere, anywhere],
            out_specs=whole((total, width)),
            scratch_shapes=[
                pltpu.VMEM((rows, width), kept.dtype),
                pltpu.VMEM((rows, width), theirs.dtype),
                pltpu.SemaphoreType.DMA((2, rows // block)),
            ],
        ),
        cost_estimate=pl.CostEstimate(
            flops=kept.size, bytes_accessed=8 * kept.size, transcendentals=0
        ),
        name="merge",
    )(jnp.stack(at).astype(jnp.int32), kept, theirs)


def merge_more_kernel(place, kept_ref, theirs_ref, base_ref, out_ref):
    theirs = theirs_ref[...].astype(jnp.float32)
    out_ref[...] = (kept_ref[...] + theirs).astype(out_ref.dtype)


def merge_more(at, kept, theirs, base, block):
    share = pl.BlockSpec((block, kept.shape[1]), lambda i, p: (i, 0))
    return pl.pallas_call(
        merge_more_kernel,
        out_shape=jax.ShapeDtypeStruct(base.shape, base.dtype),
        grid_spec=pltpu.PrefetchScalarGridSpec(
            num_scalar_prefetch=1,
            grid=(kept.shape[0] // block,),
            in_specs=[share, share, pl.BlockSpec(memory_space=pl.ANY)],
            out_specs=pl.BlockSpec((block, kept.shape[1]), lambda i, p: (p[i], 0)),
        ),
        input_output_aliases={3: 0},
        compiler_params=pltpu.CompilerParams(vmem_limit_bytes=SMALL_VMEM),
        cost_estimate=pl.CostEstimate(
            flops=kept.size, bytes_accessed=8 * kept.size, transcendentals=0
        ),
        name="merge_more",
    )(jnp.stack(at).astype(jnp.int32), kept, theirs, base)


def nearest(size):
    return sorted(range(size), key=lambda d: min(d, size - d))


def arrivals(size):
    table = []
    for z in range(size):
        order = []
        for step in range(1, size):
            if step <= z:
                order.append((0, step))
            if step <= size - 1 - z:
                order.append((1, step))
        table.append(order)
    return table


def take_kernel(runs, stride, place, in_ref, *refs):
    *outs, arrived = refs
    width = outs[0].shape[1] // runs
    first = place[0] * sum(out_ref.shape[0] for out_ref in outs)
    copies = []
    for n, out_ref in enumerate(outs):
        rows = out_ref.shape[0]
        down = pl.ds(pl.multiple_of(first, 16), rows)
        first = first + rows
        for i in range(runs):
            across = pl.ds(pl.multiple_of(i * stride + place[1] * width, width), width)
            to = out_ref.at[:, i * width : (i + 1) * width]
            sem = arrived.at[n * runs + i]
            copies.append(pltpu.make_async_copy(in_ref.at[down, across], to, sem))
    for copy in copies:
        copy.start()
    for copy in copies:
        copy.wait()


def take(tokens, place, sizes, width, stride):
    runs = tokens.shape[1] // stride
    shapes = [(size, runs * width) for size in sizes]
    return pl.pallas_call(
        lambda *refs: take_kernel(runs, stride, *refs),
        out_shape=[jax.ShapeDtypeStruct(shape, tokens.dtype) for shape in shapes],
        grid_spec=pltpu.PrefetchScalarGridSpec(
            num_scalar_prefetch=1,
            grid=(1,),
            in_specs=[pl.BlockSpec(memory_space=pl.ANY)],
            out_specs=[whole(shape) for shape in shapes],
            scratch_shapes=[pltpu.SemaphoreType.DMA((len(sizes) * runs,))],
        ),
        cost_estimate=pl.CostEstimate(
            flops=0, bytes_accessed=4 * sum(sizes) * runs * width, transcendentals=0
        ),
        name="take",
    )(place, tokens)


def chunked(rows):
    if rows % 32:
        return (rows,)
    return (rows // 2 + 16, rows // 2 - 16)


def unpack_kernel(hs, place, in_ref, out_ref):
    for head in range(out_ref.shape[0]):
        for which in range(3):
            out_ref[head, :, which * hs : (which + 1) * hs] = in_ref[
                which, :, head * hs : (head + 1) * hs
            ]


def unpack(weight, place, rows, hs):
    heads = weight.shape[2] // hs
    steps = 2 if rows % 32 == 0 else 1
    return pl.pallas_call(
        lambda *refs: unpack_kernel(hs, *refs),
        out_shape=jax.ShapeDtypeStruct((heads, rows, 3 * hs), weight.dtype),
        grid_spec=pltpu.PrefetchScalarGridSpec(
            num_scalar_prefetch=1,
            grid=(steps,),
            in_specs=[
                pl.BlockSpec(
                    (3, rows // steps, heads * hs), lambda i, p: (0, p[0] * steps + i, 0)
                )
            ],
            out_specs=pl.BlockSpec((heads, rows // steps, 3 * hs), lambda i, p: (0, i, 0)),
        ),
        cost_estimate=pl.CostEstimate(
            flops=0, bytes_accessed=12 * rows * heads * hs, transcendentals=0
        ),
        name="unpack",
    )(place, weight)


def by_head(tokens, proj_weight, cluster_ids, centroids):
    seq, heads, groups = (lax.axis_size(a) for a in ("seq", "head", "groups"))
    z, h, y = (lax.axis_index(a) for a in ("seq", "head", "groups"))
    core, x, xs = h % CORES, h // CORES, heads // CORES
    local_rows, _ = tokens.shape
    hs = centroids.shape[2]
    slice_depth = proj_weight.shape[1]
    half = slice_depth // CORES
    part = half // groups
    rows = local_rows // xs
    zero = jnp.int32(0)
    tie = lax.optimization_barrier

    def swap_core(v):
        return lax.ppermute(v, "head", [(i, i ^ 1) for i in range(heads)])

    def shift_x(v, d):
        pairs = [(i, (i // CORES + d) % xs * CORES + i % CORES) for i in range(heads)]
        return lax.ppermute(v, "head", pairs)

    def shift_y(v, d):
        return lax.ppermute(v, "groups", [(i, (i + d) % groups) for i in range(groups)])

    def shift_z(v, d):
        return lax.ppermute(v, "seq", [(i, (i + d) % seq) for i in range(seq)])

    def rightward(step):
        return [(i, i + 1) for i in range(step - 1, seq - 1)]

    def leftward(step):
        return [(i, i - 1) for i in range(1, seq - step + 1)]

    sizes = chunked(rows)
    at = jnp.stack([x, core]).astype(jnp.int32)
    mine = take(tokens, at, sizes, half, slice_depth)
    right, left = [mine], [mine]
    right.append([lax.ppermute(v, "seq", rightward(1)) for v in mine])
    left.append([lax.ppermute(v, "seq", leftward(1)) for v in mine])

    mine, weight, tokens = tie((mine, proj_weight, tokens))
    given = unpack(weight, jnp.stack([(1 - core) * groups + y]).astype(jnp.int32), part, hs)
    given = swap_core(given)
    kept = unpack(weight, jnp.stack([core * groups + y]).astype(jnp.int32), part, hs)
    at = jnp.stack([zero, core]).astype(jnp.int32)
    (own,) = take(tokens, at, (local_rows,), half, slice_depth)
    both = jnp.concatenate([kept, given], axis=2)
    member = lax.all_to_all(cluster_ids[:, :, 0], "seq", split_axis=0, concat_axis=0, tiled=True)
    id_row = member.reshape(1, seq * local_rows)
    id_col = member.reshape(seq * local_rows, 1)

    pieces = []
    for d in nearest(seq)[::-1]:
        piece = lax.dynamic_index_in_dim(both, (z + d) % seq, 0, keepdims=False)
        pieces.append((d, shift_z(piece, d) if d else piece))
    table = arrivals(seq)
    for step in range(1, seq):
        crossing = 2 * step <= seq + 1
        if step > 1 and crossing:
            for way, pairs in ((right, rightward), (left, leftward)):
                way.append([lax.ppermute(v, "seq", pairs(step)) for v in way[-1]])
        elif step > 1:
            sent, forward = [], (z >= step - 1).astype(jnp.int32)
            for ways in zip(left[-1], right[-1]):
                if sent:
                    ways, _ = tie((ways, sent[-1]))
                sent.append(choose(forward, ways))
            pairs = rightward(step) + leftward(step)
            got = [lax.ppermute(v, "seq", pairs) for v in sent]
            right.append(got)
            left.append(got)

    arrived, sources, last = [], [], None
    for k in range(seq - 1):
        picks = {}
        for at in range(seq):
            picks.setdefault(table[at][k], []).append(at)
        index, source = jnp.int32(0), jnp.int32(0)
        for i, ((direction, step), where) in enumerate(picks.items()):
            chosen = sum((z == at).astype(jnp.int32) for at in where) > 0
            index = jnp.where(chosen, i, index)
            source = jnp.where(chosen, z + (step if direction else -step), source)
        shares = [[] for _ in range(xs)]
        for chunk in range(len(sizes)):
            values = [(right, left)[direction][step][chunk] for direction, step in picks]
            if last is not None:
                values, last = tie((values, last))
            block = last = choose(index, values)
            for d in range(xs):
                shares[d].append(shift_x(block, d) if d else block)
        arrived.append(shares)
        sources.append(source)

    laid, spots = [], []
    for d, piece in pieces:
        for g in range(groups):
            laid.append(shift_y(piece, g) if g else piece)
            spots.append((z - d) % seq * groups + (y - g) % groups)
    spots = jnp.stack(spots).astype(jnp.int32)

    def place(k, d):
        return sources[k] * xs + (x - d) % xs

    early = [own] + [v for k in range(seq - 2) for share in arrived[k] for v in share]
    early_at = [z * xs + i for i in range(xs)]
    early_at += [place(k, d) for k in range(seq - 2) for d in range(xs)]
    early += arrived[-1][0]
    early_at.append(place(seq - 2, 0))
    late = [v for share in arrived[-1][1:] for v in share]
    late_at = [place(seq - 2, d) for d in range(1, xs)]

    units = 2 * sum(v.shape[0] for v in early) // rows
    tall = rows // 2 * max(n for n in range(1, units // 2 + 1) if units % n == 0)
    kept, sent = project(spots, laid, early, tall)
    theirs = swap_core(sent)
    qkv = merge(early_at, kept, theirs, seq * local_rows, rows)
    kept, sent = project(spots, laid, late, rows)
    theirs = swap_core(sent)
    qkv = merge_more(late_at, kept, theirs, qkv, rows)

    owned = centroids.shape[1]
    back = {}
    for d in nearest(seq)[::-1]:
        where = jnp.stack([(z + d) % seq]).astype(jnp.int32)
        block = attend(where, qkv, id_col, id_row, seq, owned, hs)
        back[d] = shift_z(block, d) if d else block
    sources = jnp.stack([(z - d) % seq for d in range(seq)]).astype(jnp.int32)
    pieces = [back[d] for d in range(seq)]
    context, updated = collect(sources, pieces, centroids, local_rows)
    return (context, updated)


def local(tokens, proj_weight, cluster_ids, centroids):
    seq, heads = lax.axis_size("seq"), lax.axis_size("head")
    if cluster_ids.shape[0] == seq and heads % CORES == 0:
        return by_head(tokens, proj_weight, cluster_ids, centroids)
    return routed(tokens, proj_weight, cluster_ids, centroids)


def solution(mesh):
    return jax.shard_map(
        local,
        mesh=mesh,
        in_specs=(
            P(("groups", "seq"), None),
            P(None, "seq", "head"),
            P("head", ("groups", "seq"), None),
            P(("groups", "head"), "seq", None),
        ),
        out_specs=(P(("groups", "seq"), "head"), P(("groups", "head"), "seq", None)),
        check_vma=False,
    )
```

```python
import jax
import jax.numpy as jnp
from jax import lax
from jax.experimental import pallas as pl
from jax.experimental.pallas import tpu as pltpu
from jax.sharding import PartitionSpec as P

SLOTS = 4
CORES = 2
LOG2_E = 1.4426950408889634
LINE = 4
SMALL_VMEM = 16 << 20


def routed(tokens, proj_weight, cluster_ids, centroids):
    owners = lax.axis_size("seq")
    local_rows = tokens.shape[0]
    hs = centroids.shape[2]
    clusters = centroids.shape[1] * owners
    columns = proj_weight.shape[2]
    head_count = columns // hs
    owned = clusters // owners
    capacity = owners * SLOTS
    score_scale = hs ** (-0.5)
    projected = jnp.einsum(
        "td,pdc->ptc",
        tokens,
        lax.all_gather(proj_weight, "seq", axis=1, tiled=True),
        preferred_element_type=jnp.float32,
    ).astype(jnp.bfloat16)
    per_head = projected.reshape(3, local_rows, head_count, hs).transpose(2, 1, 0, 3)
    packed = per_head.reshape(head_count, local_rows, 3 * hs)
    member = cluster_ids[:, :, 0]
    labels = jnp.arange(clusters, dtype=jnp.int32)
    onehot = (member[:, :, None] == labels[None, None, :]).astype(jnp.bfloat16)
    ordinal_rows = jnp.arange(local_rows, dtype=jnp.int32)
    earlier = (ordinal_rows[None, :] < ordinal_rows[:, None]).astype(jnp.bfloat16)
    before = jnp.einsum("ts,hsc->htc", earlier, onehot, preferred_element_type=jnp.float32)
    ranking = jnp.take_along_axis(before, member[:, :, None], axis=2)[:, :, 0].astype(jnp.int32)
    placed = member * SLOTS + ranking
    head_index = jnp.arange(head_count, dtype=jnp.int32)[:, None]
    outbox = (
        jnp.zeros((head_count, clusters * SLOTS, 3 * hs), jnp.bfloat16)
        .at[head_index, placed]
        .set(packed)
    )
    outbox = outbox.reshape(head_count, owners, owned * SLOTS, 3 * hs)
    local_counts = jnp.sum(onehot, axis=1, dtype=jnp.float32)
    tallies = local_counts.astype(jnp.int32).reshape(head_count, owners, owned)
    blocks = lax.all_to_all(outbox, "seq", split_axis=1, concat_axis=1, tiled=True)
    arrived = lax.all_to_all(tallies, "seq", split_axis=1, concat_axis=1, tiled=True)
    arranged = (
        blocks.reshape(head_count, owners, owned, SLOTS, 3 * hs)
        .transpose(0, 2, 1, 3, 4)
        .reshape(head_count, owned, capacity, 3 * hs)
    )
    filled = jnp.arange(SLOTS, dtype=jnp.int32)[None, None, None, :] < arrived[:, :, :, None]
    filled = filled.transpose(0, 2, 1, 3).reshape(head_count, owned, capacity)
    queries = arranged[:, :, :, :hs]
    key_block = arranged[:, :, :, hs : 2 * hs]
    value_block = arranged[:, :, :, 2 * hs :]
    scores = (
        jnp.einsum("hcqd,hckd->hcqk", queries, key_block, preferred_element_type=jnp.float32)
        * score_scale
    )
    ordinal = jnp.arange(capacity, dtype=jnp.int32)
    causal = ordinal[None, None, None, :] <= ordinal[None, None, :, None]
    itself = ordinal[None, None, None, :] == ordinal[None, None, :, None]
    allowed = filled[:, :, None, :] & causal | itself
    scores = jnp.where(allowed, scores, -1e30)
    row_max = jnp.max(scores, axis=3, keepdims=True)
    raised = jnp.exp(scores - row_max)
    weights = (raised / jnp.sum(raised, axis=3, keepdims=True)).astype(jnp.bfloat16)
    attended = jnp.einsum(
        "hcqk,hckd->hcqd", weights, value_block, preferred_element_type=jnp.float32
    ).astype(jnp.bfloat16)
    attended = (
        attended.reshape(head_count, owned, owners, SLOTS, hs)
        .transpose(0, 2, 1, 3, 4)
        .reshape(head_count, owners, owned * SLOTS, hs)
    )
    returned = lax.all_to_all(attended, "seq", split_axis=1, concat_axis=1, tiled=True)
    key_sums = jnp.einsum(
        "hck,hckd->hcd", filled.astype(jnp.bfloat16), key_block, preferred_element_type=jnp.float32
    )
    counts = jnp.sum(filled, axis=2).astype(jnp.float32)
    gathered = returned.reshape(head_count, clusters * SLOTS, hs)
    mine = jax.vmap(lambda table, where: table[where])(gathered, placed)
    context = mine.transpose(1, 0, 2).reshape(local_rows, head_count * hs)
    updated = 0.25 * centroids + 0.75 * key_sums / jnp.maximum(counts, 1.0)[:, :, None]
    return (context, updated)


def attend_kernel(hs, local_rows, place, qkv_ref, id_col_ref, id_row_ref, out_ref):
    rows = qkv_ref.shape[0]
    owned = out_ref.shape[0] - local_rows
    block = min(256, local_rows)
    scale = hs ** (-0.5) * LOG2_E
    at = place[0] * local_rows

    for first in range(0, local_rows, block):
        here = pl.multiple_of(at + first, block)
        queries = qkv_ref[pl.ds(here, block), :hs]
        ids = id_col_ref[pl.ds(here, block), :]

        def scores_of(start, size):
            keys = qkv_ref[pl.ds(start, size), hs : 2 * hs]
            scores = lax.dot_general(
                queries, keys, (((1,), (1,)), ((), ())), preferred_element_type=jnp.float32
            )
            return scores * scale, ids == id_row_ref[:, pl.ds(start, size)]

        def mix(raised, start, size):
            values = qkv_ref[pl.ds(start, size), 2 * hs :]
            return jnp.dot(raised.astype(jnp.bfloat16), values, preferred_element_type=jnp.float32)

        size = first + block
        base = pl.multiple_of(at, local_rows)
        scores, allowed = scores_of(base, size)
        row_at = lax.broadcasted_iota(jnp.int32, (block, size), 0) + first
        col_at = lax.broadcasted_iota(jnp.int32, (block, size), 1)
        scores = jnp.where(allowed & (col_at <= row_at), scores, -1e30)
        peak = jnp.max(scores, axis=1, keepdims=True)
        raised = jnp.exp2(scores - peak)
        total = jnp.sum(raised, axis=1, keepdims=True)
        mixed = mix(raised, base, size)

        def earlier(j, carry):
            peak, total, mixed = carry
            start = pl.multiple_of(j * local_rows, local_rows)
            scores, allowed = scores_of(start, local_rows)
            scores = jnp.where(allowed, scores, -1e30)
            higher = jnp.maximum(peak, jnp.max(scores, axis=1, keepdims=True))
            kept = jnp.exp2(peak - higher)
            raised = jnp.exp2(scores - higher)
            total = total * kept + jnp.sum(raised, axis=1, keepdims=True)
            return higher, total, mixed * kept + mix(raised, start, local_rows)

        _, total, mixed = lax.fori_loop(0, place[0], earlier, (peak, total, mixed))
        out_ref[first : first + block, :] = (mixed / total).astype(out_ref.dtype)
    label = lax.broadcasted_iota(jnp.int32, (owned, rows), 0) + place[0] * owned
    onehot = (label == id_row_ref[...]).astype(jnp.float32)
    counts = jnp.sum(onehot, axis=1, keepdims=True)
    keys = qkv_ref[:, hs : 2 * hs]
    sums = jnp.dot(onehot.astype(jnp.bfloat16), keys, preferred_element_type=jnp.float32)
    mean = 0.75 * sums / jnp.maximum(counts, 1.0)
    out_ref[local_rows:, :] = mean.astype(out_ref.dtype)


def whole(shape):
    return pl.BlockSpec(shape, lambda i, p: (0,) * len(shape))


def attend(place, qkv, id_col, id_row, seq, owned, hs):
    rows = qkv.shape[0]
    shape = (rows // seq + owned, hs)
    return pl.pallas_call(
        lambda *refs: attend_kernel(hs, rows // seq, *refs),
        out_shape=jax.ShapeDtypeStruct(shape, jnp.bfloat16),
        grid_spec=pltpu.PrefetchScalarGridSpec(
            num_scalar_prefetch=1,
            grid=(1,),
            in_specs=[whole(v.shape) for v in (qkv, id_col, id_row)],
            out_specs=whole(shape),
        ),
        compiler_params=pltpu.CompilerParams(vmem_limit_bytes=SMALL_VMEM),
        cost_estimate=pl.CostEstimate(
            flops=rows * rows * hs, bytes_accessed=rows * hs * 8, transcendentals=rows * rows // 4
        ),
        name="attend",
    )(place, qkv, id_col, id_row)


def collect_kernel(hs, local_rows, place, *refs):
    *pieces, centroid_ref, context_ref, updated_ref = refs
    for d, piece in enumerate(pieces):
        source = place[d]
        columns = pl.ds(pl.multiple_of(source * hs, hs), hs)
        context_ref[:, columns] = piece[:local_rows, :]
        mean = piece[local_rows:, :].astype(jnp.float32)
        updated_ref[source] = 0.25 * centroid_ref[source] + mean


def collect(place, pieces, centroids, local_rows):
    hs = centroids.shape[2]
    shape = (local_rows, len(pieces) * hs)
    return pl.pallas_call(
        lambda *refs: collect_kernel(hs, local_rows, *refs),
        out_shape=(
            jax.ShapeDtypeStruct(shape, jnp.bfloat16),
            jax.ShapeDtypeStruct(centroids.shape, jnp.float32),
        ),
        grid_spec=pltpu.PrefetchScalarGridSpec(
            num_scalar_prefetch=1,
            grid=(1,),
            in_specs=[whole(v.shape) for v in (*pieces, centroids)],
            out_specs=[whole(shape), whole(centroids.shape)],
        ),
        compiler_params=pltpu.CompilerParams(vmem_limit_bytes=SMALL_VMEM),
        cost_estimate=pl.CostEstimate(flops=0, bytes_accessed=1 << 20, transcendentals=0),
        name="collect",
    )(place, *pieces, centroids)


def start_one(copies, flag):
    if len(copies) == 1:
        copies[0].start()
        return
    for i, copy in enumerate(copies):

        @pl.when(flag == i)
        def _(copy=copy):
            copy.start()


def project_kernel(count, choices, spots, *refs):
    weights, refs = refs[:count], refs[count:]
    tokens = []
    for n in choices:
        tokens.append(refs[:n])
        refs = refs[n:]
    kept_ref, sent_ref, matrix, held, weight_sem, token_sem = refs
    step, flag = pl.program_id(0), spots[count]
    block, width = kept_ref.shape
    part = weights[0].shape[0]
    copies, row = {}, 0
    for i, options in enumerate(tokens):
        to = held.at[row : row + options[0].shape[0], :]
        copy = [pltpu.make_async_copy(ref, to, token_sem.at[i]) for ref in options]
        copies.setdefault(row // block, []).append(copy)
        row += options[0].shape[0]

    @pl.when(step == 0)
    def _():
        loads = []
        for i, ref in enumerate(weights):
            to = matrix.at[pl.ds(pl.multiple_of(spots[i] * part, part), part), :]
            loads.append([pltpu.make_async_copy(ref, to, weight_sem.at[i])])
        loads += copies[0]
        for copy in loads:
            start_one(copy, flag)
        for copy in loads:
            copy[0].wait()
        for at, group in copies.items():
            for copy in group if at else []:
                start_one(copy, flag)

    for at, group in copies.items():

        @pl.when(step == at)
        def _(group=group):
            for copy in group if at else []:
                copy[0].wait()

    left = held[pl.ds(pl.multiple_of(step * block, block), block), :]
    full = jnp.dot(left, matrix[...], preferred_element_type=jnp.float32)
    kept_ref[...] = full[:, :width]
    sent_ref[...] = full[:, width:].astype(sent_ref.dtype)


def project(spots, weights, tokens, block):
    tokens = [v if isinstance(v, tuple) else (v,) for v in tokens]
    depth = weights[0].shape[0] * len(weights)
    width = weights[0].shape[1] // CORES
    total = sum(v[0].shape[0] for v in tokens)
    choices = [len(v) for v in tokens]
    return pl.pallas_call(
        lambda *refs: project_kernel(len(weights), choices, *refs),
        out_shape=(
            jax.ShapeDtypeStruct((total, width), jnp.float32),
            jax.ShapeDtypeStruct((total, width), jnp.bfloat16),
        ),
        grid_spec=pltpu.PrefetchScalarGridSpec(
            num_scalar_prefetch=1,
            grid=(total // block,),
            in_specs=[pl.BlockSpec(memory_space=pl.ANY)] * (len(weights) + sum(choices)),
            out_specs=[pl.BlockSpec((block, width), lambda i, p: (i, 0))] * 2,
            scratch_shapes=[
                pltpu.VMEM((depth, CORES * width), jnp.bfloat16),
                pltpu.VMEM((total, depth), jnp.bfloat16),
                pltpu.SemaphoreType.DMA((len(weights),)),
                pltpu.SemaphoreType.DMA((len(tokens),)),
            ],
        ),
        compiler_params=pltpu.CompilerParams(dimension_semantics=("arbitrary",)),
        cost_estimate=pl.CostEstimate(
            flops=2 * total * depth * CORES * width,
            bytes_accessed=2 * depth * (total + CORES * width) + 8 * total * width,
            transcendentals=0,
        ),
        name="project",
    )(spots, *weights, *[v for options in tokens for v in options])


def merge_kernel(block, groups, place, *refs):
    sources, (out_ref, *held, sems) = refs[: 2 * groups], refs[2 * groups :]
    copies, i = [], 0
    for n in range(groups):
        for row in range(0, held[2 * n].shape[0], block):
            down = pl.ds(row, block)
            pair = [
                pltpu.make_async_copy(
                    sources[2 * n + j].at[down], held[2 * n + j].at[down], sems.at[j, i]
                )
                for j in range(2)
            ]
            for copy in pair:
                copy.start()
            copies.append((n, row, pair))
            i += 1
    for i, (n, row, pair) in enumerate(copies):
        for copy in pair:
            copy.wait()
        here = slice(row, row + block)
        both = held[2 * n][here, :] + held[2 * n + 1][here, :].astype(jnp.float32)
        to = pl.ds(pl.multiple_of(place[i] * block, block), block)
        out_ref[to, :] = both.astype(out_ref.dtype)


def merge(at, sums, total, block):
    flat = [v for pair in sums for v in pair]
    where = [i for group in at for i in group]
    width = flat[0].shape[1]
    anywhere = pl.BlockSpec(memory_space=pl.ANY)
    return pl.pallas_call(
        lambda *refs: merge_kernel(block, len(sums), *refs),
        out_shape=jax.ShapeDtypeStruct((total, width), jnp.bfloat16),
        grid_spec=pltpu.PrefetchScalarGridSpec(
            num_scalar_prefetch=1,
            grid=(1,),
            in_specs=[anywhere] * len(flat),
            out_specs=whole((total, width)),
            scratch_shapes=[pltpu.VMEM(v.shape, v.dtype) for v in flat]
            + [pltpu.SemaphoreType.DMA((2, len(where)))],
        ),
        cost_estimate=pl.CostEstimate(
            flops=total * width, bytes_accessed=8 * total * width, transcendentals=0
        ),
        name="merge",
    )(jnp.stack(where).astype(jnp.int32), *flat)


def merge_more_kernel(place, kept_ref, theirs_ref, base_ref, out_ref):
    theirs = theirs_ref[...].astype(jnp.float32)
    out_ref[...] = (kept_ref[...] + theirs).astype(out_ref.dtype)


def merge_more(at, kept, theirs, base, block):
    share = pl.BlockSpec((block, kept.shape[1]), lambda i, p: (i, 0))
    return pl.pallas_call(
        merge_more_kernel,
        out_shape=jax.ShapeDtypeStruct(base.shape, base.dtype),
        grid_spec=pltpu.PrefetchScalarGridSpec(
            num_scalar_prefetch=1,
            grid=(kept.shape[0] // block,),
            in_specs=[share, share, pl.BlockSpec(memory_space=pl.ANY)],
            out_specs=pl.BlockSpec((block, kept.shape[1]), lambda i, p: (p[i], 0)),
        ),
        input_output_aliases={3: 0},
        compiler_params=pltpu.CompilerParams(vmem_limit_bytes=SMALL_VMEM),
        cost_estimate=pl.CostEstimate(
            flops=kept.size, bytes_accessed=8 * kept.size, transcendentals=0
        ),
        name="merge_more",
    )(jnp.stack(at).astype(jnp.int32), kept, theirs, base)


def nearest(size):
    return sorted(range(size), key=lambda d: min(d, size - d))


def take_kernel(runs, stride, place, in_ref, *refs):
    *outs, arrived = refs
    width = outs[0].shape[1] // runs
    first = place[0] * sum(out_ref.shape[0] for out_ref in outs)
    copies = []
    for n, out_ref in enumerate(outs):
        rows = out_ref.shape[0]
        down = pl.ds(pl.multiple_of(first, 16), rows)
        first = first + rows
        for i in range(runs):
            across = pl.ds(pl.multiple_of(i * stride + place[1] * width, width), width)
            to = out_ref.at[:, i * width : (i + 1) * width]
            sem = arrived.at[n * runs + i]
            copies.append(pltpu.make_async_copy(in_ref.at[down, across], to, sem))
    for copy in copies:
        copy.start()
    for copy in copies:
        copy.wait()


def take(tokens, place, sizes, width, stride):
    runs = tokens.shape[1] // stride
    shapes = [(size, runs * width) for size in sizes]
    return pl.pallas_call(
        lambda *refs: take_kernel(runs, stride, *refs),
        out_shape=[jax.ShapeDtypeStruct(shape, tokens.dtype) for shape in shapes],
        grid_spec=pltpu.PrefetchScalarGridSpec(
            num_scalar_prefetch=1,
            grid=(1,),
            in_specs=[pl.BlockSpec(memory_space=pl.ANY)],
            out_specs=[whole(shape) for shape in shapes],
            scratch_shapes=[pltpu.SemaphoreType.DMA((len(sizes) * runs,))],
        ),
        cost_estimate=pl.CostEstimate(
            flops=0, bytes_accessed=4 * sum(sizes) * runs * width, transcendentals=0
        ),
        name="take",
    )(place, tokens)


def chunked(rows):
    if rows % 32:
        return (rows,)
    return (rows // 2 + 16, rows // 2 - 16)


def unpack_kernel(hs, place, in_ref, out_ref):
    for head in range(out_ref.shape[0]):
        for which in range(3):
            out_ref[head, :, which * hs : (which + 1) * hs] = in_ref[
                which, :, head * hs : (head + 1) * hs
            ]


def unpack(weight, place, rows, hs):
    heads = weight.shape[2] // hs
    steps = 2 if rows % 32 == 0 else 1
    return pl.pallas_call(
        lambda *refs: unpack_kernel(hs, *refs),
        out_shape=jax.ShapeDtypeStruct((heads, rows, 3 * hs), weight.dtype),
        grid_spec=pltpu.PrefetchScalarGridSpec(
            num_scalar_prefetch=1,
            grid=(steps,),
            in_specs=[
                pl.BlockSpec(
                    (3, rows // steps, heads * hs), lambda i, p: (0, p[0] * steps + i, 0)
                )
            ],
            out_specs=pl.BlockSpec((heads, rows // steps, 3 * hs), lambda i, p: (0, i, 0)),
        ),
        cost_estimate=pl.CostEstimate(
            flops=0, bytes_accessed=12 * rows * heads * hs, transcendentals=0
        ),
        name="unpack",
    )(place, weight)


def by_head(tokens, proj_weight, cluster_ids, centroids):
    seq, heads, groups = (lax.axis_size(a) for a in ("seq", "head", "groups"))
    z, h, y = (lax.axis_index(a) for a in ("seq", "head", "groups"))
    core, x, xs = h % CORES, h // CORES, heads // CORES
    local_rows, _ = tokens.shape
    hs = centroids.shape[2]
    slice_depth = proj_weight.shape[1]
    half = slice_depth // CORES
    part = half // groups
    rows = local_rows // xs
    zero = jnp.int32(0)
    tie = lax.optimization_barrier

    def swap_core(v):
        return lax.ppermute(v, "head", [(i, i ^ 1) for i in range(heads)])

    def shift_y(v, d):
        return lax.ppermute(v, "groups", [(i, (i + d) % groups) for i in range(groups)])

    def shift_z(v, d):
        return lax.ppermute(v, "seq", [(i, (i + d) % seq) for i in range(seq)])

    def rightward(step):
        return [(i, i + 1) for i in range(step - 1, seq - 1)]

    def leftward(step):
        return [(i, i - 1) for i in range(1, seq - step + 1)]

    sizes = chunked(rows)
    at = jnp.stack([x, core]).astype(jnp.int32)
    mine = take(tokens, at, sizes, half, slice_depth)
    right, left = [mine], [mine]
    right.append([lax.ppermute(v, "seq", rightward(1)) for v in mine])
    left.append([lax.ppermute(v, "seq", leftward(1)) for v in mine])

    mine, weight, tokens = tie((mine, proj_weight, tokens))
    given = unpack(weight, jnp.stack([(1 - core) * groups + y]).astype(jnp.int32), part, hs)
    given = swap_core(given)
    kept = unpack(weight, jnp.stack([core * groups + y]).astype(jnp.int32), part, hs)
    at = jnp.stack([zero, core]).astype(jnp.int32)
    (own,) = take(tokens, at, (local_rows,), half, slice_depth)
    both = jnp.concatenate([kept, given], axis=2)
    member = lax.all_to_all(cluster_ids[:, :, 0], "seq", split_axis=0, concat_axis=0, tiled=True)
    id_row = member.reshape(1, seq * local_rows)
    id_col = member.reshape(seq * local_rows, 1)

    pieces = []
    for d in nearest(seq)[::-1]:
        piece = lax.dynamic_index_in_dim(both, (z + d) % seq, 0, keepdims=False)
        pieces.append((d, shift_z(piece, d) if d else piece))
    inner = (z > 0) & (z < seq - 1)
    right.append([lax.ppermute(v, "seq", rightward(2)) for v in right[1]])
    left.append([lax.ppermute(v, "seq", leftward(2)) for v in left[1]])

    def chosen(flag, values, others, last=None):
        result = []
        for pair in zip(values, others):
            if last is not None:
                pair, last = tie((pair, last))
            last = jnp.where(flag, *pair)
            result.append(last)
        return result

    ends_z = (0, seq - 1)
    inner_z = range(1, seq - 1)

    def shares_x(values, where):
        pairs = [
            (at * heads + i, at * heads + (i // CORES + d) % xs * CORES + i % CORES)
            for d in range(1, xs)
            for at in where
            for i in range(heads)
        ]
        return [lax.ppermute(v, ("seq", "head"), pairs) for v in values]

    near = chosen(z == 0, left[1], right[1])
    near_x = shares_x(near, range(seq))
    other_x = shares_x(left[1], inner_z)
    far_off = chosen(z < seq // 2, left[2], right[2], near[-1])
    far_x = shares_x(far_off, range(seq))
    pairs = [(seq - 2, seq - 1), (1, 0)]
    ends = [lax.ppermute(v, "seq", pairs) for v in far_off]
    ends_x = shares_x(ends, ends_z)
    near_z = jnp.where(z == 0, 1, z - 1)
    far_z = jnp.where(z < seq // 2, z + 2, z - 2)
    last_z = jnp.where(inner, z + 1, seq - 1 - z)

    laid, spots = [], []
    for d, piece in pieces:
        for g in range(groups):
            laid.append(shift_y(piece, g) if g else piece)
            spots.append((z - d) % seq * groups + (y - g) % groups)
    spots = jnp.stack([*spots, inner]).astype(jnp.int32)

    def place(source, d):
        return source * xs + (x - d) % xs

    both_d = range(xs)
    first = [own, *near, *near_x]
    first_at = [z * xs + i for i in both_d] + [place(near_z, d) for d in both_d]
    middle = [*far_off, *far_x, *zip(ends, left[1])]
    middle_at = [place(far_z, d) for d in both_d] + [place(last_z, 0)]
    late, late_at = list(zip(ends_x, other_x)), [place(last_z, 1)]

    def projected(tokens):
        flat = [v[0] if isinstance(v, tuple) else v for v in tokens]
        units = 2 * sum(v.shape[0] for v in flat) // rows
        tall = rows // 2 * max(n for n in range(1, max(units // 2, 2) + 1) if units % n == 0)
        kept, sent = project(spots, laid, tokens, tall)
        return kept, swap_core(sent)

    sums = projected(first), projected(middle)
    qkv = merge((first_at, middle_at), sums, seq * local_rows, rows)
    kept, theirs = projected(late)
    qkv = merge_more(late_at, kept, theirs, qkv, rows)

    owned = centroids.shape[1]
    back = {}
    for d in nearest(seq)[::-1]:
        where = jnp.stack([(z + d) % seq]).astype(jnp.int32)
        block = attend(where, qkv, id_col, id_row, seq, owned, hs)
        back[d] = shift_z(block, d) if d else block
    sources = jnp.stack([(z - d) % seq for d in range(seq)]).astype(jnp.int32)
    pieces = [back[d] for d in range(seq)]
    context, updated = collect(sources, pieces, centroids, local_rows)
    return (context, updated)


def local(tokens, proj_weight, cluster_ids, centroids):
    seq, heads = lax.axis_size("seq"), lax.axis_size("head")
    if cluster_ids.shape[0] == seq == LINE and heads == 2 * CORES:
        return by_head(tokens, proj_weight, cluster_ids, centroids)
    return routed(tokens, proj_weight, cluster_ids, centroids)


def solution(mesh):
    return jax.shard_map(
        local,
        mesh=mesh,
        in_specs=(
            P(("groups", "seq"), None),
            P(None, "seq", "head"),
            P("head", ("groups", "seq"), None),
            P(("groups", "head"), "seq", None),
        ),
        out_specs=(P(("groups", "seq"), "head"), P(("groups", "head"), "seq", None)),
        check_vma=False,
    )
```

```python
import jax
import jax.numpy as jnp
from jax import lax
from jax.experimental import pallas as pl
from jax.experimental.pallas import tpu as pltpu
from jax.sharding import PartitionSpec as P

SLOTS = 4
CORES = 2
LOG2_E = 1.4426950408889634
LINE = 4
SMALL_VMEM = 16 << 20


def routed(tokens, proj_weight, cluster_ids, centroids):
    owners = lax.axis_size("seq")
    local_rows = tokens.shape[0]
    hs = centroids.shape[2]
    clusters = centroids.shape[1] * owners
    columns = proj_weight.shape[2]
    head_count = columns // hs
    owned = clusters // owners
    capacity = owners * SLOTS
    score_scale = hs ** (-0.5)
    projected = jnp.einsum(
        "td,pdc->ptc",
        tokens,
        lax.all_gather(proj_weight, "seq", axis=1, tiled=True),
        preferred_element_type=jnp.float32,
    ).astype(jnp.bfloat16)
    per_head = projected.reshape(3, local_rows, head_count, hs).transpose(2, 1, 0, 3)
    packed = per_head.reshape(head_count, local_rows, 3 * hs)
    member = cluster_ids[:, :, 0]
    labels = jnp.arange(clusters, dtype=jnp.int32)
    onehot = (member[:, :, None] == labels[None, None, :]).astype(jnp.bfloat16)
    ordinal_rows = jnp.arange(local_rows, dtype=jnp.int32)
    earlier = (ordinal_rows[None, :] < ordinal_rows[:, None]).astype(jnp.bfloat16)
    before = jnp.einsum("ts,hsc->htc", earlier, onehot, preferred_element_type=jnp.float32)
    ranking = jnp.take_along_axis(before, member[:, :, None], axis=2)[:, :, 0].astype(jnp.int32)
    placed = member * SLOTS + ranking
    head_index = jnp.arange(head_count, dtype=jnp.int32)[:, None]
    outbox = (
        jnp.zeros((head_count, clusters * SLOTS, 3 * hs), jnp.bfloat16)
        .at[head_index, placed]
        .set(packed)
    )
    outbox = outbox.reshape(head_count, owners, owned * SLOTS, 3 * hs)
    local_counts = jnp.sum(onehot, axis=1, dtype=jnp.float32)
    tallies = local_counts.astype(jnp.int32).reshape(head_count, owners, owned)
    blocks = lax.all_to_all(outbox, "seq", split_axis=1, concat_axis=1, tiled=True)
    arrived = lax.all_to_all(tallies, "seq", split_axis=1, concat_axis=1, tiled=True)
    arranged = (
        blocks.reshape(head_count, owners, owned, SLOTS, 3 * hs)
        .transpose(0, 2, 1, 3, 4)
        .reshape(head_count, owned, capacity, 3 * hs)
    )
    filled = jnp.arange(SLOTS, dtype=jnp.int32)[None, None, None, :] < arrived[:, :, :, None]
    filled = filled.transpose(0, 2, 1, 3).reshape(head_count, owned, capacity)
    queries = arranged[:, :, :, :hs]
    key_block = arranged[:, :, :, hs : 2 * hs]
    value_block = arranged[:, :, :, 2 * hs :]
    scores = (
        jnp.einsum("hcqd,hckd->hcqk", queries, key_block, preferred_element_type=jnp.float32)
        * score_scale
    )
    ordinal = jnp.arange(capacity, dtype=jnp.int32)
    causal = ordinal[None, None, None, :] <= ordinal[None, None, :, None]
    itself = ordinal[None, None, None, :] == ordinal[None, None, :, None]
    allowed = filled[:, :, None, :] & causal | itself
    scores = jnp.where(allowed, scores, -1e30)
    row_max = jnp.max(scores, axis=3, keepdims=True)
    raised = jnp.exp(scores - row_max)
    weights = (raised / jnp.sum(raised, axis=3, keepdims=True)).astype(jnp.bfloat16)
    attended = jnp.einsum(
        "hcqk,hckd->hcqd", weights, value_block, preferred_element_type=jnp.float32
    ).astype(jnp.bfloat16)
    attended = (
        attended.reshape(head_count, owned, owners, SLOTS, hs)
        .transpose(0, 2, 1, 3, 4)
        .reshape(head_count, owners, owned * SLOTS, hs)
    )
    returned = lax.all_to_all(attended, "seq", split_axis=1, concat_axis=1, tiled=True)
    key_sums = jnp.einsum(
        "hck,hckd->hcd", filled.astype(jnp.bfloat16), key_block, preferred_element_type=jnp.float32
    )
    counts = jnp.sum(filled, axis=2).astype(jnp.float32)
    gathered = returned.reshape(head_count, clusters * SLOTS, hs)
    mine = jax.vmap(lambda table, where: table[where])(gathered, placed)
    context = mine.transpose(1, 0, 2).reshape(local_rows, head_count * hs)
    updated = 0.25 * centroids + 0.75 * key_sums / jnp.maximum(counts, 1.0)[:, :, None]
    return (context, updated)


def attend_kernel(hs, local_rows, place, qkv_ref, id_col_ref, id_row_ref, out_ref):
    rows = qkv_ref.shape[0]
    owned = out_ref.shape[0] - local_rows
    block = min(512, local_rows)
    scale = hs ** (-0.5) * LOG2_E
    at = place[0] * local_rows

    for first in range(0, local_rows, block):
        here = pl.multiple_of(at + first, block)
        queries = qkv_ref[pl.ds(here, block), :hs]
        ids = id_col_ref[pl.ds(here, block), :]

        def scores_of(start, size):
            keys = qkv_ref[pl.ds(start, size), hs : 2 * hs]
            scores = lax.dot_general(
                queries, keys, (((1,), (1,)), ((), ())), preferred_element_type=jnp.float32
            )
            return scores * scale, ids == id_row_ref[:, pl.ds(start, size)]

        def mix(raised, start, size):
            values = qkv_ref[pl.ds(start, size), 2 * hs :]
            return jnp.dot(raised.astype(jnp.bfloat16), values, preferred_element_type=jnp.float32)

        size = first + block
        base = pl.multiple_of(at, local_rows)
        scores, allowed = scores_of(base, size)
        row_at = lax.broadcasted_iota(jnp.int32, (block, size), 0) + first
        col_at = lax.broadcasted_iota(jnp.int32, (block, size), 1)
        scores = jnp.where(allowed & (col_at <= row_at), scores, -1e30)
        peak = jnp.max(scores, axis=1, keepdims=True)
        raised = jnp.exp2(scores - peak)
        total = jnp.sum(raised, axis=1, keepdims=True)
        mixed = mix(raised, base, size)

        def earlier(j, carry):
            peak, total, mixed = carry
            start = pl.multiple_of(j * local_rows, local_rows)
            scores, allowed = scores_of(start, local_rows)
            scores = jnp.where(allowed, scores, -1e30)
            higher = jnp.maximum(peak, jnp.max(scores, axis=1, keepdims=True))
            kept = jnp.exp2(peak - higher)
            raised = jnp.exp2(scores - higher)
            total = total * kept + jnp.sum(raised, axis=1, keepdims=True)
            return higher, total, mixed * kept + mix(raised, start, local_rows)

        _, total, mixed = lax.fori_loop(0, place[0], earlier, (peak, total, mixed))
        out_ref[first : first + block, :] = (mixed / total).astype(out_ref.dtype)
    label = lax.broadcasted_iota(jnp.int32, (owned, rows), 0) + place[0] * owned
    onehot = (label == id_row_ref[...]).astype(jnp.float32)
    counts = jnp.sum(onehot, axis=1, keepdims=True)
    keys = qkv_ref[:, hs : 2 * hs]
    sums = jnp.dot(onehot.astype(jnp.bfloat16), keys, preferred_element_type=jnp.float32)
    mean = 0.75 * sums / jnp.maximum(counts, 1.0)
    out_ref[local_rows:, :] = mean.astype(out_ref.dtype)


def whole(shape):
    return pl.BlockSpec(shape, lambda i, p: (0,) * len(shape))


def attend(place, qkv, id_col, id_row, seq, owned, hs):
    rows = qkv.shape[0]
    shape = (rows // seq + owned, hs)
    return pl.pallas_call(
        lambda *refs: attend_kernel(hs, rows // seq, *refs),
        out_shape=jax.ShapeDtypeStruct(shape, jnp.bfloat16),
        grid_spec=pltpu.PrefetchScalarGridSpec(
            num_scalar_prefetch=1,
            grid=(1,),
            in_specs=[whole(v.shape) for v in (qkv, id_col, id_row)],
            out_specs=whole(shape),
        ),
        compiler_params=pltpu.CompilerParams(vmem_limit_bytes=SMALL_VMEM),
        cost_estimate=pl.CostEstimate(
            flops=rows * rows * hs, bytes_accessed=rows * hs * 8, transcendentals=rows * rows // 4
        ),
        name="attend",
    )(place, qkv, id_col, id_row)


def collect_kernel(hs, local_rows, place, *refs):
    *pieces, centroid_ref, context_ref, updated_ref = refs
    for d, piece in enumerate(pieces):
        source = place[d]
        columns = pl.ds(pl.multiple_of(source * hs, hs), hs)
        context_ref[:, columns] = piece[:local_rows, :]
        mean = piece[local_rows:, :].astype(jnp.float32)
        updated_ref[source] = 0.25 * centroid_ref[source] + mean


def collect(place, pieces, centroids, local_rows):
    hs = centroids.shape[2]
    shape = (local_rows, len(pieces) * hs)
    return pl.pallas_call(
        lambda *refs: collect_kernel(hs, local_rows, *refs),
        out_shape=(
            jax.ShapeDtypeStruct(shape, jnp.bfloat16),
            jax.ShapeDtypeStruct(centroids.shape, jnp.float32),
        ),
        grid_spec=pltpu.PrefetchScalarGridSpec(
            num_scalar_prefetch=1,
            grid=(1,),
            in_specs=[whole(v.shape) for v in (*pieces, centroids)],
            out_specs=[whole(shape), whole(centroids.shape)],
        ),
        compiler_params=pltpu.CompilerParams(vmem_limit_bytes=SMALL_VMEM),
        cost_estimate=pl.CostEstimate(flops=0, bytes_accessed=1 << 20, transcendentals=0),
        name="collect",
    )(place, *pieces, centroids)


def hold_kernel(in_ref, out_ref):
    for i in range(in_ref.shape[0]):
        out_ref[i] = in_ref[i]


def hold(values):
    smem = pl.BlockSpec(memory_space=pltpu.SMEM)
    return pl.pallas_call(
        hold_kernel,
        out_shape=jax.ShapeDtypeStruct(values.shape, values.dtype),
        in_specs=[smem],
        out_specs=smem,
        name="hold",
    )(values)


def start_one(copies, flag):
    if len(copies) == 1:
        copies[0].start()
        return
    for i, copy in enumerate(copies):

        @pl.when(flag == i)
        def _(copy=copy):
            copy.start()


def project_kernel(count, choices, spots, *refs):
    weights, refs = refs[:count], refs[count:]
    tokens = []
    for n in choices:
        tokens.append(refs[:n])
        refs = refs[n:]
    kept_ref, sent_ref, matrix, held, weight_sem, token_sem = refs
    step, flag = pl.program_id(0), spots[count]
    block, width = kept_ref.shape
    part = weights[0].shape[0]
    copies, row = {}, 0
    for i, options in enumerate(tokens):
        to = held.at[row : row + options[0].shape[0], :]
        copy = [pltpu.make_async_copy(ref, to, token_sem.at[i]) for ref in options]
        copies.setdefault(row // block, []).append(copy)
        row += options[0].shape[0]

    @pl.when(step == 0)
    def _():
        loads = []
        for i, ref in enumerate(weights):
            to = matrix.at[pl.ds(pl.multiple_of(spots[i] * part, part), part), :]
            loads.append([pltpu.make_async_copy(ref, to, weight_sem.at[i])])
        loads += copies[0]
        for copy in loads:
            start_one(copy, flag)
        for copy in loads:
            copy[0].wait()
        for at, group in copies.items():
            for copy in group if at else []:
                start_one(copy, flag)

    for at, group in copies.items():

        @pl.when(step == at)
        def _(group=group):
            for copy in group if at else []:
                copy[0].wait()

    left = held[pl.ds(pl.multiple_of(step * block, block), block), :]
    full = jnp.dot(left, matrix[...], preferred_element_type=jnp.float32)
    kept_ref[...] = full[:, :width]
    sent_ref[...] = full[:, width:].astype(sent_ref.dtype)


def project(spots, weights, tokens, block):
    tokens = [v if isinstance(v, tuple) else (v,) for v in tokens]
    depth = weights[0].shape[0] * len(weights)
    width = weights[0].shape[1] // CORES
    total = sum(v[0].shape[0] for v in tokens)
    choices = [len(v) for v in tokens]
    return pl.pallas_call(
        lambda *refs: project_kernel(len(weights), choices, *refs),
        out_shape=(
            jax.ShapeDtypeStruct((total, width), jnp.float32),
            jax.ShapeDtypeStruct((total, width), jnp.bfloat16),
        ),
        grid_spec=pltpu.PrefetchScalarGridSpec(
            num_scalar_prefetch=1,
            grid=(total // block,),
            in_specs=[pl.BlockSpec(memory_space=pl.ANY)] * (len(weights) + sum(choices)),
            out_specs=[pl.BlockSpec((block, width), lambda i, p: (i, 0))] * 2,
            scratch_shapes=[
                pltpu.VMEM((depth, CORES * width), jnp.bfloat16),
                pltpu.VMEM((total, depth), jnp.bfloat16),
                pltpu.SemaphoreType.DMA((len(weights),)),
                pltpu.SemaphoreType.DMA((len(tokens),)),
            ],
        ),
        compiler_params=pltpu.CompilerParams(dimension_semantics=("arbitrary",)),
        cost_estimate=pl.CostEstimate(
            flops=2 * total * depth * CORES * width,
            bytes_accessed=2 * depth * (total + CORES * width) + 8 * total * width,
            transcendentals=0,
        ),
        name="project",
    )(spots, *weights, *[v for options in tokens for v in options])


def merge_kernel(block, groups, place, *refs):
    sources, (out_ref, *held, sems) = refs[: 2 * groups], refs[2 * groups :]
    copies, i = [], 0
    for n in range(groups):
        for row in range(0, held[2 * n].shape[0], block):
            down = pl.ds(row, block)
            pair = [
                pltpu.make_async_copy(
                    sources[2 * n + j].at[down], held[2 * n + j].at[down], sems.at[j, i]
                )
                for j in range(2)
            ]
            for copy in pair:
                copy.start()
            copies.append((n, row, pair))
            i += 1
    for i, (n, row, pair) in enumerate(copies):
        for copy in pair:
            copy.wait()
        here = slice(row, row + block)
        both = held[2 * n][here, :] + held[2 * n + 1][here, :].astype(jnp.float32)
        to = pl.ds(pl.multiple_of(place[i] * block, block), block)
        out_ref[to, :] = both.astype(out_ref.dtype)


def merge(at, sums, total, block):
    flat = [v for pair in sums for v in pair]
    where = [i for group in at for i in group]
    width = flat[0].shape[1]
    anywhere = pl.BlockSpec(memory_space=pl.ANY)
    return pl.pallas_call(
        lambda *refs: merge_kernel(block, len(sums), *refs),
        out_shape=jax.ShapeDtypeStruct((total, width), jnp.bfloat16),
        grid_spec=pltpu.PrefetchScalarGridSpec(
            num_scalar_prefetch=1,
            grid=(1,),
            in_specs=[anywhere] * len(flat),
            out_specs=whole((total, width)),
            scratch_shapes=[pltpu.VMEM(v.shape, v.dtype) for v in flat]
            + [pltpu.SemaphoreType.DMA((2, len(where)))],
        ),
        cost_estimate=pl.CostEstimate(
            flops=total * width, bytes_accessed=8 * total * width, transcendentals=0
        ),
        name="merge",
    )(jnp.stack(where).astype(jnp.int32), *flat)


def merge_more_kernel(place, kept_ref, theirs_ref, base_ref, out_ref):
    theirs = theirs_ref[...].astype(jnp.float32)
    out_ref[...] = (kept_ref[...] + theirs).astype(out_ref.dtype)


def merge_more(at, kept, theirs, base, block):
    share = pl.BlockSpec((block, kept.shape[1]), lambda i, p: (i, 0))
    return pl.pallas_call(
        merge_more_kernel,
        out_shape=jax.ShapeDtypeStruct(base.shape, base.dtype),
        grid_spec=pltpu.PrefetchScalarGridSpec(
            num_scalar_prefetch=1,
            grid=(kept.shape[0] // block,),
            in_specs=[share, share, pl.BlockSpec(memory_space=pl.ANY)],
            out_specs=pl.BlockSpec((block, kept.shape[1]), lambda i, p: (p[i], 0)),
        ),
        input_output_aliases={3: 0},
        compiler_params=pltpu.CompilerParams(vmem_limit_bytes=SMALL_VMEM),
        cost_estimate=pl.CostEstimate(
            flops=kept.size, bytes_accessed=8 * kept.size, transcendentals=0
        ),
        name="merge_more",
    )(jnp.stack(at).astype(jnp.int32), kept, theirs, base)


def nearest(size):
    return sorted(range(size), key=lambda d: min(d, size - d))


def take_kernel(runs, stride, place, in_ref, *refs):
    *outs, arrived = refs
    width = outs[0].shape[1] // runs
    first = place[0] * sum(out_ref.shape[0] for out_ref in outs)
    copies = []
    for n, out_ref in enumerate(outs):
        rows = out_ref.shape[0]
        down = pl.ds(pl.multiple_of(first, 16), rows)
        first = first + rows
        for i in range(runs):
            across = pl.ds(pl.multiple_of(i * stride + place[1] * width, width), width)
            to = out_ref.at[:, i * width : (i + 1) * width]
            sem = arrived.at[n * runs + i]
            copies.append(pltpu.make_async_copy(in_ref.at[down, across], to, sem))
    for copy in copies:
        copy.start()
    for copy in copies:
        copy.wait()


def take(tokens, place, sizes, width, stride):
    runs = tokens.shape[1] // stride
    shapes = [(size, runs * width) for size in sizes]
    return pl.pallas_call(
        lambda *refs: take_kernel(runs, stride, *refs),
        out_shape=[jax.ShapeDtypeStruct(shape, tokens.dtype) for shape in shapes],
        grid_spec=pltpu.PrefetchScalarGridSpec(
            num_scalar_prefetch=1,
            grid=(1,),
            in_specs=[pl.BlockSpec(memory_space=pl.ANY)],
            out_specs=[whole(shape) for shape in shapes],
            scratch_shapes=[pltpu.SemaphoreType.DMA((len(sizes) * runs,))],
        ),
        cost_estimate=pl.CostEstimate(
            flops=0, bytes_accessed=4 * sum(sizes) * runs * width, transcendentals=0
        ),
        name="take",
    )(place, tokens)


def chunked(rows):
    if rows % 32:
        return (rows,)
    return (rows // 2 + 16, rows // 2 - 16)


def unpack_kernel(hs, place, in_ref, out_ref):
    for head in range(out_ref.shape[0]):
        for which in range(3):
            out_ref[head, :, which * hs : (which + 1) * hs] = in_ref[
                which, :, head * hs : (head + 1) * hs
            ]


def unpack(weight, place, rows, hs):
    heads = weight.shape[2] // hs
    steps = 2 if rows % 32 == 0 else 1
    return pl.pallas_call(
        lambda *refs: unpack_kernel(hs, *refs),
        out_shape=jax.ShapeDtypeStruct((heads, rows, 3 * hs), weight.dtype),
        grid_spec=pltpu.PrefetchScalarGridSpec(
            num_scalar_prefetch=1,
            grid=(steps,),
            in_specs=[
                pl.BlockSpec(
                    (3, rows // steps, heads * hs), lambda i, p: (0, p[0] * steps + i, 0)
                )
            ],
            out_specs=pl.BlockSpec((heads, rows // steps, 3 * hs), lambda i, p: (0, i, 0)),
        ),
        cost_estimate=pl.CostEstimate(
            flops=0, bytes_accessed=12 * rows * heads * hs, transcendentals=0
        ),
        name="unpack",
    )(place, weight)


def by_head(tokens, proj_weight, cluster_ids, centroids):
    seq, heads, groups = (lax.axis_size(a) for a in ("seq", "head", "groups"))
    z, h, y = (lax.axis_index(a) for a in ("seq", "head", "groups"))
    core, x, xs = h % CORES, h // CORES, heads // CORES
    local_rows, _ = tokens.shape
    hs = centroids.shape[2]
    slice_depth = proj_weight.shape[1]
    half = slice_depth // CORES
    part = half // groups
    rows = local_rows // xs
    zero = jnp.int32(0)
    tie = lax.optimization_barrier

    def swap_core(v):
        return lax.ppermute(v, "head", [(i, i ^ 1) for i in range(heads)])

    def shift_y(v, d):
        return lax.ppermute(v, "groups", [(i, (i + d) % groups) for i in range(groups)])

    def shift_z(v, d):
        return lax.ppermute(v, "seq", [(i, (i + d) % seq) for i in range(seq)])

    def rightward(step):
        return [(i, i + 1) for i in range(step - 1, seq - 1)]

    def leftward(step):
        return [(i, i - 1) for i in range(1, seq - step + 1)]

    sizes = chunked(rows)
    at = jnp.stack([x, core]).astype(jnp.int32)
    mine = take(tokens, at, sizes, half, slice_depth)
    right, left = [mine], [mine]
    right.append([lax.ppermute(v, "seq", rightward(1)) for v in mine])
    left.append([lax.ppermute(v, "seq", leftward(1)) for v in mine])

    mine, weight, tokens = tie((mine, proj_weight, tokens))
    given = unpack(weight, jnp.stack([(1 - core) * groups + y]).astype(jnp.int32), part, hs)
    given = swap_core(given)
    kept = unpack(weight, jnp.stack([core * groups + y]).astype(jnp.int32), part, hs)
    at = jnp.stack([zero, core]).astype(jnp.int32)
    (own,) = take(tokens, at, (local_rows,), half, slice_depth)
    both = jnp.concatenate([kept, given], axis=2)
    member = lax.all_to_all(cluster_ids[:, :, 0], "seq", split_axis=0, concat_axis=0, tiled=True)
    id_row = member.reshape(1, seq * local_rows)
    id_col = member.reshape(seq * local_rows, 1)

    pieces = []
    for d in nearest(seq)[::-1]:
        piece = lax.dynamic_index_in_dim(both, (z + d) % seq, 0, keepdims=False)
        pieces.append((d, shift_z(piece, d) if d else piece))
    inner = (z > 0) & (z < seq - 1)
    right.append([lax.ppermute(v, "seq", rightward(2)) for v in right[1]])
    left.append([lax.ppermute(v, "seq", leftward(2)) for v in left[1]])

    def chosen(flag, values, others, last=None):
        result = []
        for pair in zip(values, others):
            if last is not None:
                pair, last = tie((pair, last))
            last = jnp.where(flag, *pair)
            result.append(last)
        return result

    ends_z = (0, seq - 1)
    inner_z = range(1, seq - 1)

    def shares_x(values, where):
        pairs = [
            (at * heads + i, at * heads + (i // CORES + d) % xs * CORES + i % CORES)
            for d in range(1, xs)
            for at in where
            for i in range(heads)
        ]
        return [lax.ppermute(v, ("seq", "head"), pairs) for v in values]

    near = chosen(z == 0, left[1], right[1])
    near_x = shares_x(near, range(seq))
    other_x = shares_x(left[1], inner_z)
    far_off = chosen(z < seq // 2, left[2], right[2], near[-1])
    far_x = shares_x(far_off, range(seq))
    pairs = [(seq - 2, seq - 1), (1, 0)]
    ends = [lax.ppermute(v, "seq", pairs) for v in far_off]
    ends_x = shares_x(ends, ends_z)
    near_z = jnp.where(z == 0, 1, z - 1)
    far_z = jnp.where(z < seq // 2, z + 2, z - 2)
    last_z = jnp.where(inner, z + 1, seq - 1 - z)

    laid, spots = [], []
    for d, piece in pieces:
        for g in range(groups):
            laid.append(shift_y(piece, g) if g else piece)
            spots.append((z - d) % seq * groups + (y - g) % groups)
    spots = hold(jnp.stack([*spots, inner]).astype(jnp.int32))

    def place(source, d):
        return source * xs + (x - d) % xs

    both_d = range(xs)
    first = [own, *near, *near_x]
    first_at = [z * xs + i for i in both_d] + [place(near_z, d) for d in both_d]
    middle = [*far_off, *far_x, *zip(ends, left[1])]
    middle_at = [place(far_z, d) for d in both_d] + [place(last_z, 0)]
    late, late_at = list(zip(ends_x, other_x)), [place(last_z, 1)]

    def projected(tokens):
        flat = [v[0] if isinstance(v, tuple) else v for v in tokens]
        units = 2 * sum(v.shape[0] for v in flat) // rows
        tall = rows // 2 * max(n for n in range(1, max(units // 2, 2) + 1) if units % n == 0)
        kept, sent = project(spots, laid, tokens, tall)
        return kept, swap_core(sent)

    sums = projected(first), projected(middle)
    qkv = merge((first_at, middle_at), sums, seq * local_rows, rows)
    kept, theirs = projected(late)
    qkv = merge_more(late_at, kept, theirs, qkv, rows)

    owned = centroids.shape[1]
    back = {}
    for d in nearest(seq)[::-1]:
        where = jnp.stack([(z + d) % seq]).astype(jnp.int32)
        block = attend(where, qkv, id_col, id_row, seq, owned, hs)
        back[d] = shift_z(block, d) if d else block
    sources = jnp.stack([(z - d) % seq for d in range(seq)]).astype(jnp.int32)
    pieces = [back[d] for d in range(seq)]
    context, updated = collect(sources, pieces, centroids, local_rows)
    return (context, updated)


def local(tokens, proj_weight, cluster_ids, centroids):
    seq, heads = lax.axis_size("seq"), lax.axis_size("head")
    if cluster_ids.shape[0] == seq == LINE and heads == 2 * CORES:
        return by_head(tokens, proj_weight, cluster_ids, centroids)
    return routed(tokens, proj_weight, cluster_ids, centroids)


def solution(mesh):
    return jax.shard_map(
        local,
        mesh=mesh,
        in_specs=(
            P(("groups", "seq"), None),
            P(None, "seq", "head"),
            P("head", ("groups", "seq"), None),
            P(("groups", "head"), "seq", None),
        ),
        out_specs=(P(("groups", "seq"), "head"), P(("groups", "head"), "seq", None)),
        check_vma=False,
    )
```
